8 devices in a mesh: batch: 1 (over z), row: 2 (over y), col: 4 (over x, core).
Axes of the slice: x: 2, y: 2, z: 1, core: 2. Of those that a mesh axis runs over, the one named last changes fastest.
Arguments:
- tri_mat: bfloat16 [3072, 3072], P(('batch', 'row'), 'col')
- rhs_mat: bfloat16 [3072, 32768], P(('batch', 'row'), 'col')
Outputs:
- output: bfloat16 [3072, 32768], P(('batch', 'row'), 'col')
All inputs are finite; a program needn't handle non-finite values.
Results may differ from the reference program's by a relative error of at most 0.001.
Values are sent between devices in bfloat16 or wider.
A program may use at most 1 GiB of HBM per device.

```python
import jax
import jax.numpy as jnp

MAT_ORDER = 3072
BLOCK_SIZE = 256
COLS_DEV = 8192
GRID_ROWS = 2
GRID_COLS = 4
NUM_COLS = COLS_DEV * GRID_COLS
NUM_BLOCKS = MAT_ORDER // BLOCK_SIZE


def logical_index(grid_size):
    stored = jnp.arange(MAT_ORDER, dtype=jnp.int32)
    block_idx = stored // BLOCK_SIZE
    per_device = NUM_BLOCKS // grid_size
    owner_dev = block_idx // per_device
    local_blk = block_idx % per_device
    return (local_blk * grid_size + owner_dev) * BLOCK_SIZE + stored % BLOCK_SIZE


def setup_inputs(seed: int = 0, part: int = 0) -> dict:
    base_key = jax.random.fold_in(jax.random.key(seed), part)
    key_tri, key_rhs = jax.random.split(base_key)
    row_ids = logical_index(GRID_ROWS)
    col_ids = logical_index(GRID_COLS)
    lower_mask = row_ids[:, None] >= col_ids[None, :]
    scale_tri = MAT_ORDER ** -0.5
    draws = jax.random.normal(key_tri, (MAT_ORDER, MAT_ORDER), jnp.float32) * scale_tri
    tri_mat = jnp.where(lower_mask, draws, 0.0).astype(jnp.bfloat16)
    rhs_mat = jax.random.normal(key_rhs, (MAT_ORDER, NUM_COLS), jnp.float32).astype(jnp.bfloat16)
    return {"tri_mat": tri_mat, "rhs_mat": rhs_mat}


def reference(tri_mat, rhs_mat):
    by_rows = rhs_mat.reshape(GRID_ROWS, NUM_BLOCKS // GRID_ROWS, BLOCK_SIZE, NUM_COLS)
    logical = by_rows.transpose(1, 0, 2, 3).reshape(NUM_BLOCKS // GRID_COLS, GRID_COLS, BLOCK_SIZE, NUM_COLS)
    rhs_by_cols = logical.transpose(1, 0, 2, 3).reshape(MAT_ORDER, NUM_COLS)
    product = jnp.dot(tri_mat, rhs_by_cols, preferred_element_type=jnp.float32)
    return product.astype(jnp.bfloat16)
```

```python
import functools

import jax
import jax.numpy as jnp
from jax import lax
from jax.experimental import pallas as pl
from jax.experimental.pallas import tpu as pltpu
from jax.sharding import PartitionSpec as P

BLOCK = 256


def block_kernel(count, *refs):
    lo_ref, lr_ref, bo_ref = refs[:3]
    rem_refs = refs[3:3 + count]
    x_ref = refs[-1]
    acc = jnp.dot(lo_ref[...], bo_ref[...], preferred_element_type=jnp.float32)
    for j in range(count):
        acc += jnp.dot(lr_ref[:, j * BLOCK:(j + 1) * BLOCK], rem_refs[j][...], preferred_element_type=jnp.float32)
    x_ref[...] = acc.astype(x_ref.dtype)


def row_block(step, start, width, tile, l_own, l_rem, b_own, pieces, offsets, x):
    count = step + 1
    depth = count * BLOCK
    rows, cols = b_own.shape
    base = start // tile
    in_specs = [
        pl.BlockSpec((BLOCK, depth), lambda n: (step, 0)),
        pl.BlockSpec((BLOCK, depth), lambda n: (step, 0)),
        pl.BlockSpec((depth, tile), lambda n: (0, base + n)),
    ]
    for off in offsets:
        in_specs.append(pl.BlockSpec((BLOCK, tile), functools.partial(lambda shift, n: (0, shift + n), (start - off) // tile)))
    args = [l_own, l_rem, b_own, *pieces]
    aliases = {}
    if x is not None:
        aliases = {len(args): 0}
        args.append(x)
        in_specs.append(pl.BlockSpec(memory_space=pl.ANY))
    return pl.pallas_call(
        functools.partial(block_kernel, count),
        grid=(width // tile,),
        in_specs=in_specs,
        out_specs=pl.BlockSpec((BLOCK, tile), lambda n: (step, base + n)),
        out_shape=jax.ShapeDtypeStruct((rows, cols), jnp.bfloat16),
        input_output_aliases=aliases,
        compiler_params=pltpu.CompilerParams(vmem_limit_bytes=60 << 20),
        cost_estimate=pl.CostEstimate(
            flops=4 * BLOCK * depth * width, bytes_accessed=(2 * depth + BLOCK) * width * 2, transcendentals=0),
    )(*args)


def solution(mesh):
    grid_rows = mesh.shape["row"]
    grid_cols = mesh.shape["col"]
    swap_row = [(r, r ^ 1) for r in range(grid_rows)]
    swap_core = [(c, c ^ 1) for c in range(grid_cols)]
    swap_chip = [(c, c ^ 2) for c in range(grid_cols)]

    def local_trmm(tri_loc, rhs_loc):
        rows, cols = rhs_loc.shape
        steps = rows // BLOCK
        tail = [cols // 2, cols // 4, cols // 8, cols // 8]

        rem = [lax.ppermute(rhs_loc[j * BLOCK:(j + 1) * BLOCK], "row", swap_row) for j in range(steps - 1)]
        last, off = [], 0
        for w in tail:
            last.append((off, w, lax.ppermute(rhs_loc[(steps - 1) * BLOCK:, off:off + w], "row", swap_row)))
            off += w

        l_core = lax.ppermute(tri_loc, "col", swap_core)
        l_chip = lax.ppermute(tri_loc, "col", swap_chip)
        l_both = lax.ppermute(l_chip, "col", swap_core)
        p = lax.axis_index("row")
        q = lax.axis_index("col")
        order = jnp.arange(grid_cols) ^ q
        l_all = jnp.stack([tri_loc, l_core, l_chip, l_both])[order]
        l_all = l_all.reshape(2, 2, rows, steps // 2, BLOCK)
        l_par = l_all.transpose(1, 2, 3, 0, 4).reshape(2, rows, rows)
        l_own, l_rem = l_par[p], l_par[1 - p]

        x = None
        for j in range(steps - 1):
            x = row_block(j, 0, cols, 1024, l_own, l_rem, rhs_loc, rem[:j + 1], [0] * (j + 1), x)
        for off, w, piece in last:
            x = row_block(steps - 1, off, w, min(1024, w), l_own, l_rem, rhs_loc, [*rem, piece], [0] * (steps - 1) + [off], x)
        return x

    part_spec = P(("batch", "row"), "col")
    return jax.shard_map(local_trmm, mesh=mesh, in_specs=(part_spec, part_spec), out_specs=part_spec, check_vma=False)
```

```python
import functools

import jax
import jax.numpy as jnp
from jax import lax
from jax.experimental import pallas as pl
from jax.experimental.pallas import tpu as pltpu
from jax.sharding import PartitionSpec as P


BLOCK = 256


def block_kernel(count, *refs):
    lo_ref, lr_ref, bo_ref = refs[:3]
    rem_refs = refs[3:3 + count]
    out_ref = refs[-1]
    acc = jnp.dot(lo_ref[...], bo_ref[...], preferred_element_type=jnp.float32)
    for j in range(count):
        acc += jnp.dot(lr_ref[:, j * BLOCK:(j + 1) * BLOCK], rem_refs[j][...], preferred_element_type=jnp.float32)
    out_ref[...] = acc.astype(out_ref.dtype)


def row_block(step, count, start, tile, l_own, l_rem, b_own, pieces, x, partial=False):
    depth = (step + 1) * BLOCK
    rows, cols = b_own.shape
    width = pieces[0].shape[1]
    base = start // tile
    in_specs = [
        pl.BlockSpec((BLOCK, depth), lambda n: (step, 0)),
        pl.BlockSpec((BLOCK, count * BLOCK), lambda n: (step, 0)),
        pl.BlockSpec((depth, tile), lambda n: (0, base + n)),
    ]
    in_specs += [pl.BlockSpec((BLOCK, tile), lambda n: (0, n))] * count
    args = [l_own, l_rem, b_own, *pieces[:count]]
    aliases = {}
    if partial:
        out_spec = pl.BlockSpec((BLOCK, tile), lambda n: (0, n))
        out_shape = jax.ShapeDtypeStruct((BLOCK, width), jnp.float32)
    else:
        out_spec = pl.BlockSpec((BLOCK, tile), lambda n: (step, base + n))
        out_shape = jax.ShapeDtypeStruct((rows, cols), jnp.bfloat16)
        if x is not None:
            aliases = {len(args): 0}
            args.append(x)
            in_specs.append(pl.BlockSpec(memory_space=pl.ANY))
    return pl.pallas_call(
        functools.partial(block_kernel, count),
        grid=(width // tile,),
        in_specs=in_specs,
        out_specs=out_spec,
        out_shape=out_shape,
        input_output_aliases=aliases,
        compiler_params=pltpu.CompilerParams(vmem_limit_bytes=40 << 20),
        cost_estimate=pl.CostEstimate(
            flops=2 * BLOCK * (depth + count * BLOCK) * width,
            bytes_accessed=(depth + count * BLOCK + BLOCK) * width * 2, transcendentals=0),
    )(*args)


def finish_kernel(l_ref, b_ref, acc_ref, x_in, x_ref):
    del x_in
    acc = acc_ref[...] + jnp.dot(l_ref[...], b_ref[...], preferred_element_type=jnp.float32)
    x_ref[...] = acc.astype(x_ref.dtype)


def finish(step, start, tile, l_rem, piece, acc, acc_start, x):
    width = piece.shape[1]
    base, acc_base = start // tile, acc_start // tile
    return pl.pallas_call(
        finish_kernel,
        grid=(width // tile,),
        in_specs=[
            pl.BlockSpec((BLOCK, BLOCK), lambda n: (step, step)),
            pl.BlockSpec((BLOCK, tile), lambda n: (0, n)),
            pl.BlockSpec((BLOCK, tile), lambda n: (0, acc_base + n)),
            pl.BlockSpec(memory_space=pl.ANY),
        ],
        out_specs=pl.BlockSpec((BLOCK, tile), lambda n: (step, base + n)),
        out_shape=jax.ShapeDtypeStruct(x.shape, x.dtype),
        input_output_aliases={3: 0},
        compiler_params=pltpu.CompilerParams(vmem_limit_bytes=16 << 20),
        cost_estimate=pl.CostEstimate(
            flops=2 * BLOCK * BLOCK * width, bytes_accessed=BLOCK * width * 8, transcendentals=0),
    )(l_rem, piece, acc, x)


def weave(even, odd):
    count = even.shape[1] // BLOCK
    parts = []
    for j in range(count):
        parts += [even[:, j * BLOCK:(j + 1) * BLOCK], odd[:, j * BLOCK:(j + 1) * BLOCK]]
    return jnp.concatenate(parts, axis=1)


def solution(mesh):
    grid_rows = mesh.shape["row"]
    grid_cols = mesh.shape["col"]
    swap_row = [(r, r ^ 1) for r in range(grid_rows)]

    def local_trmm(tri_loc, rhs_loc):
        rows, cols = rhs_loc.shape
        steps = rows // BLOCK
        final = steps - 1
        half = cols // 2
        first = cols // 16

        order = [(final, cols - first, first)]
        order += [(j, h * half, half) for j in range(final) for h in range(2)]
        tail = [(0, half), (half, cols // 4), (half + cols // 4, cols // 8), (cols - 2 * first, first)]
        order += [(final, off, w) for off, w in tail]

        got = {}
        source = rhs_loc
        for j, off, w in order:
            piece = source[j * BLOCK:(j + 1) * BLOCK, off:off + w]
            source, piece = lax.optimization_barrier((source, piece))
            got[j, off] = lax.ppermute(piece, "row", swap_row)
        l_core, l_chip, l_both = (
            lax.ppermute(tri_loc, "col", [(c, c ^ d) for c in range(grid_cols)]) for d in (1, 2, 3))
        p = lax.axis_index("row")
        q = lax.axis_index("col")
        on_first = q < 2
        same = weave(jnp.where(on_first, tri_loc, l_chip), jnp.where(on_first, l_chip, tri_loc))
        other = weave(jnp.where(on_first, l_core, l_both), jnp.where(on_first, l_both, l_core))
        matches = (q % 2) == p
        l_own = jnp.where(matches, same, other)
        l_rem = jnp.where(matches, other, same)

        x = None
        for j in range(final):
            for h in range(2):
                x = row_block(j, j + 1, h * half, 1024, l_own, l_rem, rhs_loc, [got[k, h * half] for k in range(j + 1)], x)
        acc = [row_block(final, final, h * half, 1024, l_own, l_rem, rhs_loc, [got[k, h * half] for k in range(final)], None,
                         partial=True) for h in range(2)]
        for off, w in [(cols - first, first), *tail]:
            h = off // half
            x = finish(final, off, min(w, 1024), l_rem, got[final, off], acc[h], off - h * half, x)
        return x

    part_spec = P(("batch", "row"), "col")
    return jax.shard_map(local_trmm, mesh=mesh, in_specs=(part_spec, part_spec), out_specs=part_spec, check_vma=False)
```

```python
import functools

import jax
import jax.numpy as jnp
from jax import lax
from jax.experimental import pallas as pl
from jax.experimental.pallas import tpu as pltpu
from jax.sharding import PartitionSpec as P


BLOCK = 256


def block_kernel(count, aliased, *refs):
    lo_ref, lr_ref, bo_ref = refs[:3]
    rem_refs = refs[3:3 + count]
    out_refs = refs[3 + count + aliased:]
    acc = jnp.dot(lo_ref[...], bo_ref[...], preferred_element_type=jnp.float32)
    for j in range(count):
        acc += jnp.dot(lr_ref[:, j * BLOCK:(j + 1) * BLOCK], rem_refs[j][...], preferred_element_type=jnp.float32)
    for out_ref in out_refs:
        out_ref[...] = acc.astype(out_ref.dtype)


def row_block(step, count, start, tile, l_own, l_rem, b_own, pieces, x, partial=False):
    depth = (step + 1) * BLOCK
    rows, cols = b_own.shape
    width = pieces[0].shape[1]
    base = start // tile
    in_specs = [
        pl.BlockSpec((BLOCK, depth), lambda n: (step, 0)),
        pl.BlockSpec((BLOCK, count * BLOCK), lambda n: (step, 0)),
        pl.BlockSpec((depth, tile), lambda n: (0, base + n)),
    ]
    in_specs += [pl.BlockSpec((BLOCK, tile), lambda n: (0, n))] * count
    args = [l_own, l_rem, b_own, *pieces[:count]]
    out_specs = [pl.BlockSpec((BLOCK, tile), lambda n: (step, base + n))]
    out_shape = [jax.ShapeDtypeStruct((rows, cols), jnp.bfloat16)]
    aliases = {}
    if x is not None:
        aliases = {len(args): 0}
        args.append(x)
        in_specs.append(pl.BlockSpec(memory_space=pltpu.HBM))
    if partial:
        out_specs.append(pl.BlockSpec((BLOCK, tile), lambda n: (0, n)))
        out_shape.append(jax.ShapeDtypeStruct((BLOCK, width), jnp.float32))
    return pl.pallas_call(
        functools.partial(block_kernel, count, len(aliases)),
        grid=(width // tile,),
        in_specs=in_specs,
        out_specs=out_specs,
        out_shape=out_shape,
        input_output_aliases=aliases,
        compiler_params=pltpu.CompilerParams(vmem_limit_bytes=40 << 20),
        cost_estimate=pl.CostEstimate(
            flops=2 * BLOCK * (depth + count * BLOCK) * width,
            bytes_accessed=(depth + count * BLOCK + BLOCK) * width * 2, transcendentals=0),
    )(*args)


def finish_kernel(step, start, row, tile, acc_start, l_ref, b_ref, acc_ref, x_in, x_ref, l_buf, b_buf, acc_buf, out_buf, sems):
    del x_in
    rows = pl.ds(step * BLOCK, BLOCK)

    @pl.when(lax.axis_index("row") == row)
    def _():
        l_copy = pltpu.make_async_copy(l_ref.at[rows, rows], l_buf, sems.at[0])
        b_copy = pltpu.make_async_copy(b_ref, b_buf, sems.at[1])
        acc_copy = pltpu.make_async_copy(acc_ref.at[:, pl.ds(acc_start, b_ref.shape[1])], acc_buf, sems.at[2])
        l_copy.start()
        b_copy.start()
        acc_copy.start()
        l_copy.wait()
        b_copy.wait()
        acc_copy.wait()

        @pl.loop(0, b_ref.shape[1] // tile)
        def _(n):
            columns = pl.ds(pl.multiple_of(n * tile, tile), tile)
            acc = acc_buf[:, columns] + jnp.dot(l_buf[...], b_buf[:, columns], preferred_element_type=jnp.float32)
            out_buf[:, columns] = acc.astype(out_buf.dtype)

        out_copy = pltpu.make_async_copy(out_buf, x_ref.at[rows, pl.ds(start, b_ref.shape[1])], sems.at[3])
        out_copy.start()
        out_copy.wait()


def finish(step, start, row, l_rem, piece, acc, acc_start, x):
    width = piece.shape[1]
    return pl.pallas_call(
        functools.partial(finish_kernel, step, start, row, min(width, 512), acc_start),
        in_specs=[pl.BlockSpec(memory_space=pltpu.HBM)] * 4,
        out_specs=pl.BlockSpec(memory_space=pltpu.HBM),
        out_shape=jax.ShapeDtypeStruct(x.shape, x.dtype),
        scratch_shapes=[
            pltpu.VMEM((BLOCK, BLOCK), l_rem.dtype),
            pltpu.VMEM((BLOCK, width), piece.dtype),
            pltpu.VMEM((BLOCK, width), acc.dtype),
            pltpu.VMEM((BLOCK, width), x.dtype),
            pltpu.SemaphoreType.DMA((4,)),
        ],
        input_output_aliases={3: 0},
        compiler_params=pltpu.CompilerParams(vmem_limit_bytes=16 << 20),
        cost_estimate=pl.CostEstimate(
            flops=2 * BLOCK * BLOCK * width, bytes_accessed=BLOCK * width * 8, transcendentals=0),
    )(l_rem, piece, acc, x)


def weave(even, odd):
    count = even.shape[1] // BLOCK
    parts = []
    for j in range(count):
        parts += [even[:, j * BLOCK:(j + 1) * BLOCK], odd[:, j * BLOCK:(j + 1) * BLOCK]]
    return jnp.concatenate(parts, axis=1)


def solution(mesh):
    grid_rows = mesh.shape["row"]
    grid_cols = mesh.shape["col"]
    swap_row = [(r, r ^ 1) for r in range(grid_rows)]

    def local_trmm(tri_loc, rhs_loc):
        rows, cols = rhs_loc.shape
        steps = rows // BLOCK
        final = steps - 1
        half = cols // 2
        first = cols // 16

        order = [(final, cols - first, first)]
        order += [(j, h * half, half) for j in range(final) for h in range(2)]
        tail = [(0, half), (half, cols // 4), (half + cols // 4, cols // 8), (cols - 2 * first, first)]
        order += [(final, off, w) for off, w in tail]

        got = {}
        source = rhs_loc
        for j, off, w in order:
            piece = source[j * BLOCK:(j + 1) * BLOCK, off:off + w]
            source, piece = lax.optimization_barrier((source, piece))
            got[j, off] = lax.ppermute(piece, "row", swap_row)
        l_core, l_chip, l_both = (
            lax.ppermute(tri_loc, "col", [(c, c ^ d) for c in range(grid_cols)]) for d in (1, 2, 3))
        p = lax.axis_index("row")
        q = lax.axis_index("col")
        on_first = q < 2
        same = weave(jnp.where(on_first, tri_loc, l_chip), jnp.where(on_first, l_chip, tri_loc))
        other = weave(jnp.where(on_first, l_core, l_both), jnp.where(on_first, l_both, l_core))
        matches = (q % 2) == p
        l_own = jnp.where(matches, same, other)
        l_rem = jnp.where(matches, other, same)

        x = None
        for j in range(final):
            for h in range(2):
                x, = row_block(j, j + 1, h * half, 1024, l_own, l_rem, rhs_loc, [got[k, h * half] for k in range(j + 1)], x)
        acc = [None, None]
        for h in range(2):
            x, acc[h] = row_block(
                final, final, h * half, 1024, l_own, l_rem, rhs_loc, [got[k, h * half] for k in range(final)], x, partial=True)
        for off, w in [(cols - first, first), *tail]:
            h = off // half
            x = finish(final, off, grid_rows - 1, l_rem, got[final, off], acc[h], off - h * half, x)
        return x

    part_spec = P(("batch", "row"), "col")
    return jax.shard_map(local_trmm, mesh=mesh, in_specs=(part_spec, part_spec), out_specs=part_spec, check_vma=False)
```

```python
import functools

import jax
import jax.numpy as jnp
from jax import lax
from jax.experimental import pallas as pl
from jax.experimental.pallas import tpu as pltpu
from jax.sharding import PartitionSpec as P


BLOCK = 256


def block_kernel(count, aliased, *refs):
    lo_ref, lr_ref, bo_ref = refs[:3]
    rem_refs = refs[3:3 + count]
    out_refs = refs[3 + count + aliased:]
    acc = jnp.dot(lo_ref[...], bo_ref[...], preferred_element_type=jnp.float32)
    for j in range(count):
        acc += jnp.dot(lr_ref[:, j * BLOCK:(j + 1) * BLOCK], rem_refs[j][...], preferred_element_type=jnp.float32)
    for out_ref in out_refs:
        out_ref[...] = acc.astype(out_ref.dtype)


def row_block(step, count, start, tile, l_own, l_rem, b_own, pieces, x, partial=False):
    depth = (step + 1) * BLOCK
    rows, cols = b_own.shape
    width = pieces[0].shape[1]
    base = start // tile
    in_specs = [
        pl.BlockSpec((BLOCK, depth), lambda n: (step, 0)),
        pl.BlockSpec((BLOCK, count * BLOCK), lambda n: (step, 0)),
        pl.BlockSpec((depth, tile), lambda n: (0, base + n)),
    ]
    in_specs += [pl.BlockSpec((BLOCK, tile), lambda n: (0, n))] * count
    args = [l_own, l_rem, b_own, *pieces[:count]]
    out_specs = [pl.BlockSpec((BLOCK, tile), lambda n: (step, base + n))]
    out_shape = [jax.ShapeDtypeStruct((rows, cols), jnp.bfloat16)]
    aliases = {}
    if x is not None:
        aliases = {len(args): 0}
        args.append(x)
        in_specs.append(pl.BlockSpec(memory_space=pltpu.HBM))
    if partial:
        out_specs.append(pl.BlockSpec((BLOCK, tile), lambda n: (0, n)))
        out_shape.append(jax.ShapeDtypeStruct((BLOCK, width), jnp.float32))
    return pl.pallas_call(
        functools.partial(block_kernel, count, len(aliases)),
        grid=(width // tile,),
        in_specs=in_specs,
        out_specs=out_specs,
        out_shape=out_shape,
        input_output_aliases=aliases,
        compiler_params=pltpu.CompilerParams(vmem_limit_bytes=40 << 20),
        cost_estimate=pl.CostEstimate(
            flops=2 * BLOCK * (depth + count * BLOCK) * width,
            bytes_accessed=(depth + count * BLOCK + BLOCK) * width * 2, transcendentals=0),
    )(*args)


def finish_kernel(step, start, row, tile, acc_start, l_ref, b_ref, acc_ref, x_in, x_ref, l_buf, b_buf, acc_buf, out_buf, sems):
    del x_in
    rows = pl.ds(step * BLOCK, BLOCK)

    @pl.when(lax.axis_index("row") == row)
    def _():
        l_copy = pltpu.make_async_copy(l_ref.at[rows, rows], l_buf, sems.at[0])
        b_copy = pltpu.make_async_copy(b_ref, b_buf, sems.at[1])
        acc_copy = pltpu.make_async_copy(acc_ref.at[:, pl.ds(acc_start, b_ref.shape[1])], acc_buf, sems.at[2])
        l_copy.start()
        b_copy.start()
        acc_copy.start()
        l_copy.wait()
        b_copy.wait()
        acc_copy.wait()

        @pl.loop(0, b_ref.shape[1] // tile)
        def _(n):
            columns = pl.ds(pl.multiple_of(n * tile, tile), tile)
            acc = acc_buf[:, columns] + jnp.dot(l_buf[...], b_buf[:, columns], preferred_element_type=jnp.float32)
            out_buf[:, columns] = acc.astype(out_buf.dtype)

        out_copy = pltpu.make_async_copy(out_buf, x_ref.at[rows, pl.ds(start, b_ref.shape[1])], sems.at[3])
        out_copy.start()
        out_copy.wait()


def finish(step, start, row, l_rem, piece, acc, acc_start, x):
    width = piece.shape[1]
    return pl.pallas_call(
        functools.partial(finish_kernel, step, start, row, min(width, 512), acc_start),
        in_specs=[pl.BlockSpec(memory_space=pltpu.HBM)] * 4,
        out_specs=pl.BlockSpec(memory_space=pltpu.HBM),
        out_shape=jax.ShapeDtypeStruct(x.shape, x.dtype),
        scratch_shapes=[
            pltpu.VMEM((BLOCK, BLOCK), l_rem.dtype),
            pltpu.VMEM((BLOCK, width), piece.dtype),
            pltpu.VMEM((BLOCK, width), acc.dtype),
            pltpu.VMEM((BLOCK, width), x.dtype),
            pltpu.SemaphoreType.DMA((4,)),
        ],
        input_output_aliases={3: 0},
        compiler_params=pltpu.CompilerParams(vmem_limit_bytes=16 << 20),
        cost_estimate=pl.CostEstimate(
            flops=2 * BLOCK * BLOCK * width, bytes_accessed=BLOCK * width * 8, transcendentals=0),
    )(l_rem, piece, acc, x)


def cut_kernel(row, start, b_ref, out_ref, buf, sems):
    @pl.when(lax.axis_index("row") == 0)
    def _():
        fetch = pltpu.make_async_copy(b_ref.at[pl.ds(row, BLOCK), pl.ds(start, buf.shape[1])], buf, sems.at[0])
        fetch.start()
        fetch.wait()
        store = pltpu.make_async_copy(buf, out_ref, sems.at[1])
        store.start()
        store.wait()


def cut(b, row, start, width):
    return pl.pallas_call(
        functools.partial(cut_kernel, row, start),
        in_specs=[pl.BlockSpec(memory_space=pltpu.HBM)],
        out_specs=pl.BlockSpec(memory_space=pltpu.HBM),
        out_shape=jax.ShapeDtypeStruct((BLOCK, width), b.dtype),
        scratch_shapes=[pltpu.VMEM((BLOCK, width), b.dtype), pltpu.SemaphoreType.DMA((2,))],
        compiler_params=pltpu.CompilerParams(vmem_limit_bytes=60 << 20),
        cost_estimate=pl.CostEstimate(flops=2 * BLOCK * width, bytes_accessed=BLOCK * width * 4, transcendentals=0),
    )(b)


def weave(even, odd):
    count = even.shape[1] // BLOCK
    parts = []
    for j in range(count):
        parts += [even[:, j * BLOCK:(j + 1) * BLOCK], odd[:, j * BLOCK:(j + 1) * BLOCK]]
    return jnp.concatenate(parts, axis=1)


def solution(mesh):
    grid_rows = mesh.shape["row"]
    grid_cols = mesh.shape["col"]
    swap_row = [(r, r ^ 1) for r in range(grid_rows)]
    down_row = [(r, r + 1) for r in range(grid_rows - 1)]

    def local_trmm(tri_loc, rhs_loc):
        rows, cols = rhs_loc.shape
        steps = rows // BLOCK
        final = steps - 1
        half = cols // 2
        first = cols // 16

        order = [(final, cols - first, first)]
        order += [(j, h * half, half) for j in range(final) for h in range(2)]
        tail = [(0, half), (half, cols // 4), (half + cols // 4, cols // 8), (cols - 2 * first, first)]
        order += [(final, off, w) for off, w in tail]

        got = {}
        source = rhs_loc
        for i, (j, off, w) in enumerate(order):
            piece = source[j * BLOCK:(j + 1) * BLOCK, off:off + w] if i else cut(source, j * BLOCK, off, w)
            source, piece = lax.optimization_barrier((source, piece))
            got[j, off] = lax.ppermute(piece, "row", down_row if i and j == final else swap_row)
        l_core, l_chip, l_both = (
            lax.ppermute(tri_loc, "col", [(c, c ^ d) for c in range(grid_cols)]) for d in (1, 2, 3))
        p = lax.axis_index("row")
        q = lax.axis_index("col")
        on_first = q < 2
        same = weave(jnp.where(on_first, tri_loc, l_chip), jnp.where(on_first, l_chip, tri_loc))
        other = weave(jnp.where(on_first, l_core, l_both), jnp.where(on_first, l_both, l_core))
        matches = (q % 2) == p
        l_own = jnp.where(matches, same, other)
        l_rem = jnp.where(matches, other, same)

        x = None
        for j in range(final):
            for h in range(2):
                x, = row_block(j, j + 1, h * half, 1024, l_own, l_rem, rhs_loc, [got[k, h * half] for k in range(j + 1)], x)
        acc = [None, None]
        for h in range(2):
            x, acc[h] = row_block(
                final, final, h * half, 1024, l_own, l_rem, rhs_loc, [got[k, h * half] for k in range(final)], x, partial=True)
        for off, w in [(cols - first, first), *tail]:
            h = off // half
            x = finish(final, off, grid_rows - 1, l_rem, got[final, off], acc[h], off - h * half, x)
        return x

    part_spec = P(("batch", "row"), "col")
    return jax.shard_map(local_trmm, mesh=mesh, in_specs=(part_spec, part_spec), out_specs=part_spec, check_vma=False)
```

```python
import functools

import jax
import jax.numpy as jnp
from jax import lax
from jax.experimental import pallas as pl
from jax.experimental.pallas import tpu as pltpu
from jax.sharding import PartitionSpec as P


BLOCK = 256


def block_kernel(count, aliased, *refs):
    lo_ref, lr_ref, bo_ref = refs[:3]
    rem_refs = refs[3:3 + count]
    out_refs = refs[3 + count + aliased:]
    acc = jnp.dot(lo_ref[...], bo_ref[...], preferred_element_type=jnp.float32)
    for j in range(count):
        acc += jnp.dot(lr_ref[:, j * BLOCK:(j + 1) * BLOCK], rem_refs[j][...], preferred_element_type=jnp.float32)
    for out_ref in out_refs:
        out_ref[...] = acc.astype(out_ref.dtype)


def row_block(step, count, start, tile, l_own, l_rem, b_own, pieces, x, partial=False):
    depth = (step + 1) * BLOCK
    rows, cols = b_own.shape
    width = pieces[0].shape[1]
    base = start // tile
    in_specs = [
        pl.BlockSpec((BLOCK, depth), lambda n: (step, 0)),
        pl.BlockSpec((BLOCK, count * BLOCK), lambda n: (step, 0)),
        pl.BlockSpec((depth, tile), lambda n: (0, base + n)),
    ]
    in_specs += [pl.BlockSpec((BLOCK, tile), lambda n: (0, n))] * count
    args = [l_own, l_rem, b_own, *pieces[:count]]
    out_specs = [pl.BlockSpec((BLOCK, tile), lambda n: (step, base + n))]
    out_shape = [jax.ShapeDtypeStruct((rows, cols), jnp.bfloat16)]
    aliases = {}
    if x is not None:
        aliases = {len(args): 0}
        args.append(x)
        in_specs.append(pl.BlockSpec(memory_space=pltpu.HBM))
    if partial:
        out_specs.append(pl.BlockSpec((BLOCK, tile), lambda n: (0, n)))
        out_shape.append(jax.ShapeDtypeStruct((BLOCK, width), jnp.float32))
    return pl.pallas_call(
        functools.partial(block_kernel, count, len(aliases)),
        grid=(width // tile,),
        in_specs=in_specs,
        out_specs=out_specs,
        out_shape=out_shape,
        input_output_aliases=aliases,
        compiler_params=pltpu.CompilerParams(vmem_limit_bytes=24 << 20),
        cost_estimate=pl.CostEstimate(
            flops=2 * BLOCK * (depth + count * BLOCK) * width,
            bytes_accessed=(depth + count * BLOCK + BLOCK) * width * 2, transcendentals=0),
    )(*args)


def finish_kernel(step, start, row, tile, acc_start, l_ref, b_ref, acc_ref, x_in, x_ref, l_buf, b_buf, acc_buf, out_buf, sems):
    del x_in
    rows = pl.ds(step * BLOCK, BLOCK)

    @pl.when(lax.axis_index("row") == row)
    def _():
        l_copy = pltpu.make_async_copy(l_ref.at[rows, rows], l_buf, sems.at[0])
        b_copy = pltpu.make_async_copy(b_ref, b_buf, sems.at[1])
        acc_copy = pltpu.make_async_copy(acc_ref.at[:, pl.ds(acc_start, b_ref.shape[1])], acc_buf, sems.at[2])
        l_copy.start()
        b_copy.start()
        acc_copy.start()
        l_copy.wait()
        b_copy.wait()
        acc_copy.wait()

        @pl.loop(0, b_ref.shape[1] // tile)
        def _(n):
            columns = pl.ds(pl.multiple_of(n * tile, tile), tile)
            acc = acc_buf[:, columns] + jnp.dot(l_buf[...], b_buf[:, columns], preferred_element_type=jnp.float32)
            out_buf[:, columns] = acc.astype(out_buf.dtype)

        out_copy = pltpu.make_async_copy(out_buf, x_ref.at[rows, pl.ds(start, b_ref.shape[1])], sems.at[3])
        out_copy.start()
        out_copy.wait()


def finish(step, start, row, l_rem, piece, acc, acc_start, x):
    width = piece.shape[1]
    return pl.pallas_call(
        functools.partial(finish_kernel, step, start, row, min(width, 512), acc_start),
        in_specs=[pl.BlockSpec(memory_space=pltpu.HBM)] * 4,
        out_specs=pl.BlockSpec(memory_space=pltpu.HBM),
        out_shape=jax.ShapeDtypeStruct(x.shape, x.dtype),
        scratch_shapes=[
            pltpu.VMEM((BLOCK, BLOCK), l_rem.dtype),
            pltpu.VMEM((BLOCK, width), piece.dtype),
            pltpu.VMEM((BLOCK, width), acc.dtype),
            pltpu.VMEM((BLOCK, width), x.dtype),
            pltpu.SemaphoreType.DMA((4,)),
        ],
        input_output_aliases={3: 0},
        compiler_params=pltpu.CompilerParams(vmem_limit_bytes=12 << 20),
        cost_estimate=pl.CostEstimate(
            flops=2 * BLOCK * BLOCK * width, bytes_accessed=BLOCK * width * 8, transcendentals=0),
    )(l_rem, piece, acc, x)


def last_kernel(step, start, row, l_ref, b_ref, acc_ref, x_in, x_ref, out_buf, sem):
    del x_in

    @pl.when(lax.axis_index("row") == row)
    def _():
        acc = acc_ref[...] + jnp.dot(l_ref[...], b_ref[...], preferred_element_type=jnp.float32)
        out_buf[...] = acc.astype(out_buf.dtype)
        copy = pltpu.make_async_copy(
            out_buf, x_ref.at[pl.ds(step * BLOCK, BLOCK), pl.ds(start, b_ref.shape[1])], sem)
        copy.start()
        copy.wait()


def finish_last(step, start, row, l_last, piece, acc, x):
    width = piece.shape[1]
    return pl.pallas_call(
        functools.partial(last_kernel, step, start, row),
        in_specs=[pl.BlockSpec(memory_space=pltpu.VMEM)] * 3 + [pl.BlockSpec(memory_space=pltpu.HBM)],
        out_specs=pl.BlockSpec(memory_space=pltpu.HBM),
        out_shape=jax.ShapeDtypeStruct(x.shape, x.dtype),
        scratch_shapes=[pltpu.VMEM((BLOCK, width), x.dtype), pltpu.SemaphoreType.DMA],
        input_output_aliases={3: 0},
        compiler_params=pltpu.CompilerParams(vmem_limit_bytes=8 << 20),
        cost_estimate=pl.CostEstimate(
            flops=2 * BLOCK * BLOCK * width, bytes_accessed=BLOCK * width * 8, transcendentals=0),
    )(l_last, piece, acc, x)


def cut_kernel(row, start, b_ref, out_ref, buf, sems):
    @pl.when(lax.axis_index("row") == 0)
    def _():
        fetch = pltpu.make_async_copy(b_ref.at[pl.ds(row, BLOCK), pl.ds(start, buf.shape[1])], buf, sems.at[0])
        fetch.start()
        fetch.wait()
        store = pltpu.make_async_copy(buf, out_ref, sems.at[1])
        store.start()
        store.wait()


def cut(b, row, start, width):
    return pl.pallas_call(
        functools.partial(cut_kernel, row, start),
        in_specs=[pl.BlockSpec(memory_space=pltpu.HBM)],
        out_specs=pl.BlockSpec(memory_space=pltpu.HBM),
        out_shape=jax.ShapeDtypeStruct((BLOCK, width), b.dtype),
        scratch_shapes=[pltpu.VMEM((BLOCK, width), b.dtype), pltpu.SemaphoreType.DMA((2,))],
        compiler_params=pltpu.CompilerParams(vmem_limit_bytes=60 << 20),
        cost_estimate=pl.CostEstimate(flops=2 * BLOCK * width, bytes_accessed=BLOCK * width * 4, transcendentals=0),
    )(b)


def weave(even, odd):
    count = even.shape[1] // BLOCK
    parts = []
    for j in range(count):
        parts += [even[:, j * BLOCK:(j + 1) * BLOCK], odd[:, j * BLOCK:(j + 1) * BLOCK]]
    return jnp.concatenate(parts, axis=1)


def solution(mesh):
    grid_rows = mesh.shape["row"]
    grid_cols = mesh.shape["col"]
    swap_row = [(r, r ^ 1) for r in range(grid_rows)]
    down_row = [(r, r + 1) for r in range(grid_rows - 1)]

    def local_trmm(tri_loc, rhs_loc):
        rows, cols = rhs_loc.shape
        steps = rows // BLOCK
        final = steps - 1
        half = cols // 2
        first = cols // 16

        order = [(final, cols - first, first)]
        order += [(j, h * half, half) for j in range(final) for h in range(2)]
        tail = [(0, half), (half, cols // 4), (half + cols // 4, cols // 8), (cols - 2 * first, first)]
        order += [(final, off, w) for off, w in tail]

        got = {}

        def send(i, source):
            j, off, w = order[i]
            piece = source[j * BLOCK:(j + 1) * BLOCK, off:off + w] if i else cut(source, j * BLOCK, off, w)
            source, piece = lax.optimization_barrier((source, piece))
            got[j, off] = lax.ppermute(piece, "row", down_row if i and j == final else swap_row)
            return source

        source = rhs_loc
        for i in range(len(order) - 1):
            source = send(i, source)
        l_core, l_chip, l_both = (
            lax.ppermute(tri_loc, "col", [(c, c ^ d) for c in range(grid_cols)]) for d in (1, 2, 3))
        p = lax.axis_index("row")
        q = lax.axis_index("col")
        on_first = q < 2
        same = weave(jnp.where(on_first, tri_loc, l_chip), jnp.where(on_first, l_chip, tri_loc))
        other = weave(jnp.where(on_first, l_core, l_both), jnp.where(on_first, l_both, l_core))
        matches = (q % 2) == p
        l_own = jnp.where(matches, same, other)
        l_rem = jnp.where(matches, other, same)

        x = None
        for j in range(final):
            for h in range(2):
                x, = row_block(j, j + 1, h * half, 1024, l_own, l_rem, rhs_loc, [got[k, h * half] for k in range(j + 1)], x)
        acc = [None, None]
        for h in range(2):
            x, acc[h] = row_block(
                final, final, h * half, 1024, l_own, l_rem, rhs_loc, [got[k, h * half] for k in range(final)], x, partial=True)
        l_last = l_rem[final * BLOCK:, final * BLOCK:]
        off, w = tail[-1]
        acc_last = acc[1][:, off - half:off - half + w]
        source, acc[1] = lax.optimization_barrier((source, acc[1]))
        send(len(order) - 1, source)
        for off, w in [(cols - first, first), *tail[:-1]]:
            h = off // half
            x = finish(final, off, grid_rows - 1, l_rem, got[final, off], acc[h], off - h * half, x)
        off, w = tail[-1]
        return finish_last(final, off, grid_rows - 1, l_last, got[final, off], acc_last, x)

    part_spec = P(("batch", "row"), "col")
    return jax.shard_map(local_trmm, mesh=mesh, in_specs=(part_spec, part_spec), out_specs=part_spec, check_vma=False)
```

```python
import functools

import jax
import jax.numpy as jnp
from jax import lax
from jax.experimental import pallas as pl
from jax.experimental.pallas import tpu as pltpu
from jax.sharding import PartitionSpec as P


BLOCK = 256


def block_kernel(count, aliased, *refs):
    lo_ref, lr_ref, bo_ref = refs[:3]
    rem_refs = refs[3:3 + count]
    out_refs = refs[3 + count + aliased:]
    acc = jnp.dot(lo_ref[...], bo_ref[...], preferred_element_type=jnp.float32)
    for j in range(count):
        acc += jnp.dot(lr_ref[:, j * BLOCK:(j + 1) * BLOCK], rem_refs[j][...], preferred_element_type=jnp.float32)
    for out_ref in out_refs:
        out_ref[...] = acc.astype(out_ref.dtype)


def row_block(step, count, start, tile, l_own, l_rem, b_own, pieces, x, partial=False):
    depth = (step + 1) * BLOCK
    rows, cols = b_own.shape
    width = pieces[0].shape[1]
    base = start // tile
    in_specs = [
        pl.BlockSpec((BLOCK, depth), lambda n: (step, 0)),
        pl.BlockSpec((BLOCK, count * BLOCK), lambda n: (step, 0)),
        pl.BlockSpec((depth, tile), lambda n: (0, base + n)),
    ]
    in_specs += [pl.BlockSpec((BLOCK, tile), lambda n: (0, n))] * count
    args = [l_own, l_rem, b_own, *pieces[:count]]
    out_specs = [pl.BlockSpec((BLOCK, tile), lambda n: (step, base + n))]
    out_shape = [jax.ShapeDtypeStruct((rows, cols), jnp.bfloat16)]
    aliases = {}
    if x is not None:
        aliases = {len(args): 0}
        args.append(x)
        in_specs.append(pl.BlockSpec(memory_space=pltpu.HBM))
    if partial:
        out_specs.append(pl.BlockSpec((BLOCK, tile), lambda n: (0, n)))
        out_shape.append(jax.ShapeDtypeStruct((BLOCK, width), jnp.float32))
    return pl.pallas_call(
        functools.partial(block_kernel, count, len(aliases)),
        grid=(width // tile,),
        in_specs=in_specs,
        out_specs=out_specs,
        out_shape=out_shape,
        input_output_aliases=aliases,
        compiler_params=pltpu.CompilerParams(vmem_limit_bytes=24 << 20),
        cost_estimate=pl.CostEstimate(
            flops=2 * BLOCK * (depth + count * BLOCK) * width,
            bytes_accessed=(depth + count * BLOCK + BLOCK) * width * 2, transcendentals=0),
    )(*args)


def finish_kernel(step, start, row, tile, acc_start, l_ref, b_ref, acc_ref, x_in, x_ref, l_buf, b_buf, acc_buf, out_buf, sems):
    del x_in
    rows = pl.ds(step * BLOCK, BLOCK)

    @pl.when(lax.axis_index("row") == row)
    def _():
        l_copy = pltpu.make_async_copy(l_ref.at[rows, rows], l_buf, sems.at[0])
        b_copy = pltpu.make_async_copy(b_ref, b_buf, sems.at[1])
        acc_copy = pltpu.make_async_copy(acc_ref.at[:, pl.ds(acc_start, b_ref.shape[1])], acc_buf, sems.at[2])
        l_copy.start()
        b_copy.start()
        acc_copy.start()
        l_copy.wait()
        b_copy.wait()
        acc_copy.wait()

        @pl.loop(0, b_ref.shape[1] // tile)
        def _(n):
            columns = pl.ds(pl.multiple_of(n * tile, tile), tile)
            acc = acc_buf[:, columns] + jnp.dot(l_buf[...], b_buf[:, columns], preferred_element_type=jnp.float32)
            out_buf[:, columns] = acc.astype(out_buf.dtype)

        out_copy = pltpu.make_async_copy(out_buf, x_ref.at[rows, pl.ds(start, b_ref.shape[1])], sems.at[3])
        out_copy.start()
        out_copy.wait()


def finish(step, start, row, l_rem, piece, acc, acc_start, x):
    width = piece.shape[1]
    return pl.pallas_call(
        functools.partial(finish_kernel, step, start, row, min(width, 512), acc_start),
        in_specs=[pl.BlockSpec(memory_space=pltpu.HBM)] * 4,
        out_specs=pl.BlockSpec(memory_space=pltpu.HBM),
        out_shape=jax.ShapeDtypeStruct(x.shape, x.dtype),
        scratch_shapes=[
            pltpu.VMEM((BLOCK, BLOCK), l_rem.dtype),
            pltpu.VMEM((BLOCK, width), piece.dtype),
            pltpu.VMEM((BLOCK, width), acc.dtype),
            pltpu.VMEM((BLOCK, width), x.dtype),
            pltpu.SemaphoreType.DMA((4,)),
        ],
        input_output_aliases={3: 0},
        compiler_params=pltpu.CompilerParams(vmem_limit_bytes=12 << 20),
        cost_estimate=pl.CostEstimate(
            flops=2 * BLOCK * BLOCK * width, bytes_accessed=BLOCK * width * 8, transcendentals=0),
    )(l_rem, piece, acc, x)


def last_kernel(step, start, row, l_ref, b_ref, acc_ref, x_in, x_ref, out_buf, sem):
    del x_in

    @pl.when(lax.axis_index("row") == row)
    def _():
        acc = acc_ref[...] + jnp.dot(l_ref[...], b_ref[...], preferred_element_type=jnp.float32)
        out_buf[...] = acc.astype(out_buf.dtype)
        copy = pltpu.make_async_copy(
            out_buf, x_ref.at[pl.ds(step * BLOCK, BLOCK), pl.ds(start, b_ref.shape[1])], sem)
        copy.start()
        copy.wait()


def finish_last(step, start, row, l_last, piece, acc, x):
    width = piece.shape[1]
    return pl.pallas_call(
        functools.partial(last_kernel, step, start, row),
        in_specs=[pl.BlockSpec(memory_space=pltpu.VMEM)] * 3 + [pl.BlockSpec(memory_space=pltpu.HBM)],
        out_specs=pl.BlockSpec(memory_space=pltpu.HBM),
        out_shape=jax.ShapeDtypeStruct(x.shape, x.dtype),
        scratch_shapes=[pltpu.VMEM((BLOCK, width), x.dtype), pltpu.SemaphoreType.DMA],
        input_output_aliases={3: 0},
        compiler_params=pltpu.CompilerParams(vmem_limit_bytes=8 << 20),
        cost_estimate=pl.CostEstimate(
            flops=2 * BLOCK * BLOCK * width, bytes_accessed=BLOCK * width * 8, transcendentals=0),
    )(l_last, piece, acc, x)


def cut_kernel(row, start, b_ref, out_ref, sem):
    @pl.when(lax.axis_index("row") == 0)
    def _():
        copy = pltpu.make_async_copy(b_ref.at[pl.ds(row, BLOCK), pl.ds(start, out_ref.shape[1])], out_ref, sem)
        copy.start()
        copy.wait()


def cut(b, row, start, width):
    return pl.pallas_call(
        functools.partial(cut_kernel, row, start),
        in_specs=[pl.BlockSpec(memory_space=pltpu.HBM)],
        out_specs=pl.BlockSpec(memory_space=pl.ANY),
        out_shape=jax.ShapeDtypeStruct((BLOCK, width), b.dtype),
        scratch_shapes=[pltpu.SemaphoreType.DMA],
        compiler_params=pltpu.CompilerParams(vmem_limit_bytes=48 << 20),
        cost_estimate=pl.CostEstimate(flops=2 * BLOCK * width, bytes_accessed=BLOCK * width * 4, transcendentals=0),
    )(b)


def keep_kernel(row, piece_ref, out_ref, sem):
    @pl.when(lax.axis_index("row") == row)
    def _():
        copy = pltpu.make_async_copy(piece_ref, out_ref, sem)
        copy.start()
        copy.wait()


def keep(row, piece):
    return pl.pallas_call(
        functools.partial(keep_kernel, row),
        in_specs=[pl.BlockSpec(memory_space=pltpu.VMEM)],
        out_specs=pl.BlockSpec(memory_space=pltpu.HBM),
        out_shape=jax.ShapeDtypeStruct(piece.shape, piece.dtype),
        scratch_shapes=[pltpu.SemaphoreType.DMA],
        compiler_params=pltpu.CompilerParams(vmem_limit_bytes=1 << 20),
        cost_estimate=pl.CostEstimate(flops=2 * piece.size, bytes_accessed=4 * piece.size, transcendentals=0),
    )(piece)


def weave(even, odd):
    count = even.shape[1] // BLOCK
    parts = []
    for j in range(count):
        parts += [even[:, j * BLOCK:(j + 1) * BLOCK], odd[:, j * BLOCK:(j + 1) * BLOCK]]
    return jnp.concatenate(parts, axis=1)


def solution(mesh):
    grid_rows = mesh.shape["row"]
    grid_cols = mesh.shape["col"]
    swap_row = [(r, r ^ 1) for r in range(grid_rows)]
    down_row = [(r, r + 1) for r in range(grid_rows - 1)]

    def local_trmm(tri_loc, rhs_loc):
        rows, cols = rhs_loc.shape
        steps = rows // BLOCK
        final = steps - 1
        half = cols // 2
        first = cols // 16

        order = [(final, cols - first, first)]
        order += [(j, h * half, half) for j in range(final) for h in range(2)]
        tail = [(0, half), (half, cols // 4), (half + cols // 4, cols // 8), (cols - 2 * first, first)]
        order += [(final, off, w) for off, w in tail]

        got = {}

        def send(i, source):
            j, off, w = order[i]
            piece = source[j * BLOCK:(j + 1) * BLOCK, off:off + w] if i else cut(source, j * BLOCK, off, w)
            source, piece = lax.optimization_barrier((source, piece))
            got[j, off] = lax.ppermute(piece, "row", down_row if i and j == final else swap_row)
            return source

        source = rhs_loc
        for i in range(len(order) - 1):
            source = send(i, source)
        got[final, cols - first] = keep(grid_rows - 1, got[final, cols - first])
        l_core, l_chip, l_both = (
            lax.ppermute(tri_loc, "col", [(c, c ^ d) for c in range(grid_cols)]) for d in (1, 2, 3))
        p = lax.axis_index("row")
        q = lax.axis_index("col")
        on_first = q < 2
        same = weave(jnp.where(on_first, tri_loc, l_chip), jnp.where(on_first, l_chip, tri_loc))
        other = weave(jnp.where(on_first, l_core, l_both), jnp.where(on_first, l_both, l_core))
        matches = (q % 2) == p
        l_own = jnp.where(matches, same, other)
        l_rem = jnp.where(matches, other, same)

        x = None
        for j in range(final):
            for h in range(2):
                x, = row_block(j, j + 1, h * half, 1024, l_own, l_rem, rhs_loc, [got[k, h * half] for k in range(j + 1)], x)
        acc = [None, None]
        for h in range(2):
            x, acc[h] = row_block(
                final, final, h * half, 1024, l_own, l_rem, rhs_loc, [got[k, h * half] for k in range(final)], x, partial=True)
        l_last = l_rem[final * BLOCK:, final * BLOCK:]
        off, w = tail[-1]
        acc_last = acc[1][:, off - half:off - half + w]
        source, acc[1] = lax.optimization_barrier((source, acc[1]))
        send(len(order) - 1, source)
        for off, w in [(cols - first, first), *tail[:-1]]:
            h = off // half
            x = finish(final, off, grid_rows - 1, l_rem, got[final, off], acc[h], off - h * half, x)
        off, w = tail[-1]
        return finish_last(final, off, grid_rows - 1, l_last, got[final, off], acc_last, x)

    part_spec = P(("batch", "row"), "col")
    return jax.shard_map(local_trmm, mesh=mesh, in_specs=(part_spec, part_spec), out_specs=part_spec, check_vma=False)
```

```python
import functools

import jax
import jax.numpy as jnp
from jax import lax
from jax.experimental import pallas as pl
from jax.experimental.pallas import tpu as pltpu
from jax.sharding import PartitionSpec as P


BLOCK = 256


def bulk_kernel(steps, aliased, lo_ref, lr_ref, bo_ref, *refs):
    rem_refs = refs[:steps - 1]
    x_ref, acc_ref = refs[steps - 1 + aliased:]
    for step in range(steps):
        rows = slice(step * BLOCK, (step + 1) * BLOCK)
        depth = (step + 1) * BLOCK
        acc = jnp.dot(lo_ref[rows, :depth], bo_ref[:depth, :], preferred_element_type=jnp.float32)
        for j in range(min(step + 1, steps - 1)):
            columns = slice(j * BLOCK, (j + 1) * BLOCK)
            acc += jnp.dot(lr_ref[rows, columns], rem_refs[j][...], preferred_element_type=jnp.float32)
        x_ref[rows, :] = acc.astype(x_ref.dtype)
    acc_ref[...] = acc


def bulk(start, tile, l_own, l_rem, b_own, pieces, x):
    rows, cols = b_own.shape
    steps = rows // BLOCK
    width = pieces[0].shape[1]
    base = start // tile
    whole = pl.BlockSpec((rows, rows), lambda n: (0, 0), pipeline_mode=pl.Buffered(1))
    column = pl.BlockSpec((rows, tile), lambda n: (0, base + n))
    in_specs = [whole, whole, column] + [pl.BlockSpec((BLOCK, tile), lambda n: (0, n))] * (steps - 1)
    args = [l_own, l_rem, b_own, *pieces]
    aliases = {}
    if x is not None:
        aliases = {len(args): 0}
        args.append(x)
        in_specs.append(pl.BlockSpec(memory_space=pltpu.HBM))
    return pl.pallas_call(
        functools.partial(bulk_kernel, steps, len(aliases)),
        grid=(width // tile,),
        in_specs=in_specs,
        out_specs=[column, pl.BlockSpec((BLOCK, tile), lambda n: (0, n))],
        out_shape=[jax.ShapeDtypeStruct((rows, cols), jnp.bfloat16), jax.ShapeDtypeStruct((BLOCK, width), jnp.float32)],
        input_output_aliases=aliases,
        compiler_params=pltpu.CompilerParams(vmem_limit_bytes=32 << 20),
        cost_estimate=pl.CostEstimate(
            flops=2 * rows * rows * width, bytes_accessed=3 * rows * width * 2, transcendentals=0),
    )(*args)


def finish_kernel(step, start, row, tile, acc_start, l_ref, b_ref, acc_ref, x_in, x_ref, l_buf, b_buf, acc_buf, out_buf, sems):
    del x_in
    rows = pl.ds(step * BLOCK, BLOCK)

    @pl.when(lax.axis_index("row") == row)
    def _():
        l_copy = pltpu.make_async_copy(l_ref.at[rows, rows], l_buf, sems.at[0])
        b_copy = pltpu.make_async_copy(b_ref, b_buf, sems.at[1])
        acc_copy = pltpu.make_async_copy(acc_ref.at[:, pl.ds(acc_start, b_ref.shape[1])], acc_buf, sems.at[2])
        l_copy.start()
        b_copy.start()
        acc_copy.start()
        l_copy.wait()
        b_copy.wait()
        acc_copy.wait()

        @pl.loop(0, b_ref.shape[1] // tile)
        def _(n):
            columns = pl.ds(pl.multiple_of(n * tile, tile), tile)
            acc = acc_buf[:, columns] + jnp.dot(l_buf[...], b_buf[:, columns], preferred_element_type=jnp.float32)
            out_buf[:, columns] = acc.astype(out_buf.dtype)

        out_copy = pltpu.make_async_copy(out_buf, x_ref.at[rows, pl.ds(start, b_ref.shape[1])], sems.at[3])
        out_copy.start()
        out_copy.wait()


def finish(step, start, row, l_rem, piece, acc, acc_start, x):
    width = piece.shape[1]
    return pl.pallas_call(
        functools.partial(finish_kernel, step, start, row, min(width, 512), acc_start),
        in_specs=[pl.BlockSpec(memory_space=pltpu.HBM)] * 4,
        out_specs=pl.BlockSpec(memory_space=pltpu.HBM),
        out_shape=jax.ShapeDtypeStruct(x.shape, x.dtype),
        scratch_shapes=[
            pltpu.VMEM((BLOCK, BLOCK), l_rem.dtype),
            pltpu.VMEM((BLOCK, width), piece.dtype),
            pltpu.VMEM((BLOCK, width), acc.dtype),
            pltpu.VMEM((BLOCK, width), x.dtype),
            pltpu.SemaphoreType.DMA((4,)),
        ],
        input_output_aliases={3: 0},
        compiler_params=pltpu.CompilerParams(vmem_limit_bytes=12 << 20),
        cost_estimate=pl.CostEstimate(
            flops=2 * BLOCK * BLOCK * width, bytes_accessed=BLOCK * width * 8, transcendentals=0),
    )(l_rem, piece, acc, x)


def last_kernel(step, start, row, l_ref, b_ref, acc_ref, x_in, x_ref, out_buf, sem):
    del x_in

    @pl.when(lax.axis_index("row") == row)
    def _():
        acc = acc_ref[...] + jnp.dot(l_ref[...], b_ref[...], preferred_element_type=jnp.float32)
        out_buf[...] = acc.astype(out_buf.dtype)
        copy = pltpu.make_async_copy(
            out_buf, x_ref.at[pl.ds(step * BLOCK, BLOCK), pl.ds(start, b_ref.shape[1])], sem)
        copy.start()
        copy.wait()


def finish_last(step, start, row, l_last, piece, acc, x):
    width = piece.shape[1]
    return pl.pallas_call(
        functools.partial(last_kernel, step, start, row),
        in_specs=[pl.BlockSpec(memory_space=pltpu.VMEM)] * 3 + [pl.BlockSpec(memory_space=pltpu.HBM)],
        out_specs=pl.BlockSpec(memory_space=pltpu.HBM),
        out_shape=jax.ShapeDtypeStruct(x.shape, x.dtype),
        scratch_shapes=[pltpu.VMEM((BLOCK, width), x.dtype), pltpu.SemaphoreType.DMA],
        input_output_aliases={3: 0},
        compiler_params=pltpu.CompilerParams(vmem_limit_bytes=8 << 20),
        cost_estimate=pl.CostEstimate(
            flops=2 * BLOCK * BLOCK * width, bytes_accessed=BLOCK * width * 8, transcendentals=0),
    )(l_last, piece, acc, x)


def cut_kernel(row, start, b_ref, out_ref, sem):
    @pl.when(lax.axis_index("row") == 0)
    def _():
        copy = pltpu.make_async_copy(b_ref.at[pl.ds(row, BLOCK), pl.ds(start, out_ref.shape[1])], out_ref, sem)
        copy.start()
        copy.wait()


def cut(b, row, start, width):
    return pl.pallas_call(
        functools.partial(cut_kernel, row, start),
        in_specs=[pl.BlockSpec(memory_space=pltpu.HBM)],
        out_specs=pl.BlockSpec(memory_space=pl.ANY),
        out_shape=jax.ShapeDtypeStruct((BLOCK, width), b.dtype),
        scratch_shapes=[pltpu.SemaphoreType.DMA],
        compiler_params=pltpu.CompilerParams(vmem_limit_bytes=48 << 20),
        cost_estimate=pl.CostEstimate(flops=2 * BLOCK * width, bytes_accessed=BLOCK * width * 4, transcendentals=0),
    )(b)


def keep_kernel(row, piece_ref, out_ref, sem):
    @pl.when(lax.axis_index("row") == row)
    def _():
        copy = pltpu.make_async_copy(piece_ref, out_ref, sem)
        copy.start()
        copy.wait()


def keep(row, piece):
    return pl.pallas_call(
        functools.partial(keep_kernel, row),
        in_specs=[pl.BlockSpec(memory_space=pltpu.VMEM)],
        out_specs=pl.BlockSpec(memory_space=pltpu.HBM),
        out_shape=jax.ShapeDtypeStruct(piece.shape, piece.dtype),
        scratch_shapes=[pltpu.SemaphoreType.DMA],
        compiler_params=pltpu.CompilerParams(vmem_limit_bytes=1 << 20),
        cost_estimate=pl.CostEstimate(flops=2 * piece.size, bytes_accessed=4 * piece.size, transcendentals=0),
    )(piece)


def weave(even, odd):
    count = even.shape[1] // BLOCK
    parts = []
    for j in range(count):
        parts += [even[:, j * BLOCK:(j + 1) * BLOCK], odd[:, j * BLOCK:(j + 1) * BLOCK]]
    return jnp.concatenate(parts, axis=1)


def solution(mesh):
    grid_rows = mesh.shape["row"]
    grid_cols = mesh.shape["col"]
    swap_row = [(r, r ^ 1) for r in range(grid_rows)]
    down_row = [(r, r + 1) for r in range(grid_rows - 1)]

    def local_trmm(tri_loc, rhs_loc):
        rows, cols = rhs_loc.shape
        steps = rows // BLOCK
        final = steps - 1
        half = cols // 2
        first = cols // 16

        order = [(final, cols - first, first)]
        order += [(j, h * half, half) for j in range(final) for h in range(2)]
        tail = [(0, half), (half, cols // 4), (half + cols // 4, cols // 8), (cols - 2 * first, first)]
        order += [(final, off, w) for off, w in tail]

        got = {}

        def send(i, source):
            j, off, w = order[i]
            piece = source[j * BLOCK:(j + 1) * BLOCK, off:off + w] if i else cut(source, j * BLOCK, off, w)
            source, piece = lax.optimization_barrier((source, piece))
            got[j, off] = lax.ppermute(piece, "row", down_row if i and j == final else swap_row)
            return source

        source = rhs_loc
        for i in range(len(order) - 1):
            source = send(i, source)
        got[final, cols - first] = keep(grid_rows - 1, got[final, cols - first])
        l_core, l_chip, l_both = (
            lax.ppermute(tri_loc, "col", [(c, c ^ d) for c in range(grid_cols)]) for d in (1, 2, 3))
        p = lax.axis_index("row")
        q = lax.axis_index("col")
        on_first = q < 2
        same = weave(jnp.where(on_first, tri_loc, l_chip), jnp.where(on_first, l_chip, tri_loc))
        other = weave(jnp.where(on_first, l_core, l_both), jnp.where(on_first, l_both, l_core))
        matches = (q % 2) == p
        l_own = jnp.where(matches, same, other)
        l_rem = jnp.where(matches, other, same)

        x, acc = None, [None, None]
        for h in range(2):
            x, acc[h] = bulk(h * half, 512, l_own, l_rem, rhs_loc, [got[k, h * half] for k in range(final)], x)
        l_last = l_rem[final * BLOCK:, final * BLOCK:]
        off, w = tail[-1]
        acc_last = acc[1][:, off - half:off - half + w]
        source, acc[1] = lax.optimization_barrier((source, acc[1]))
        send(len(order) - 1, source)
        for off, w in [(cols - first, first), *tail[:-1]]:
            h = off // half
            x = finish(final, off, grid_rows - 1, l_rem, got[final, off], acc[h], off - h * half, x)
        off, w = tail[-1]
        return finish_last(final, off, grid_rows - 1, l_last, got[final, off], acc_last, x)

    part_spec = P(("batch", "row"), "col")
    return jax.shard_map(local_trmm, mesh=mesh, in_specs=(part_spec, part_spec), out_specs=part_spec, check_vma=False)
```

```python
import functools

import jax
import jax.numpy as jnp
from jax import lax
from jax.experimental import pallas as pl
from jax.experimental.pallas import tpu as pltpu
from jax.sharding import PartitionSpec as P


BLOCK = 256


def bulk_kernel(steps, aliased, *refs):
    l_refs, bo_ref, rem_refs = refs[:4], refs[4], refs[5:4 + steps]
    x_ref, acc_ref, last_ref, l_buf, sems = refs[4 + steps + aliased:]

    @pl.when(pl.program_id(0) == 0)
    def _():
        row, col = lax.axis_index("row"), lax.axis_index("col")
        copies = []
        for d in range(4):
            chip, core = (col // 2 + d // 2) % 2, (col + d) % 2
            side = (core + row) % 2
            for j in range(steps // 2):
                place = pl.multiple_of((2 * j + chip) * BLOCK, BLOCK)
                copies.append(pltpu.make_async_copy(
                    l_refs[d].at[:, pl.ds(j * BLOCK, BLOCK)], l_buf.at[side, :, pl.ds(place, BLOCK)], sems.at[len(copies)]))
        for copy in copies:
            copy.start()
        for copy in copies:
            copy.wait()
        last_ref[...] = l_buf[1, (steps - 1) * BLOCK:, (steps - 1) * BLOCK:]

    for step in range(steps):
        rows = slice(step * BLOCK, (step + 1) * BLOCK)
        depth = (step + 1) * BLOCK
        acc = jnp.dot(l_buf[0, rows, :depth], bo_ref[:depth, :], preferred_element_type=jnp.float32)
        for j in range(min(step + 1, steps - 1)):
            columns = slice(j * BLOCK, (j + 1) * BLOCK)
            acc += jnp.dot(l_buf[1, rows, columns], rem_refs[j][...], preferred_element_type=jnp.float32)
        x_ref[rows, :] = acc.astype(x_ref.dtype)
    acc_ref[...] = acc


def bulk(start, tile, l_parts, b_own, pieces, x):
    rows, cols = b_own.shape
    steps = rows // BLOCK
    width = pieces[0].shape[1]
    base = start // tile
    column = pl.BlockSpec((rows, tile), lambda n: (0, base + n))
    in_specs = [pl.BlockSpec(memory_space=pltpu.HBM)] * 4 + [column]
    in_specs += [pl.BlockSpec((BLOCK, tile), lambda n: (0, n))] * (steps - 1)
    args = [*l_parts, b_own, *pieces]
    aliases = {}
    if x is not None:
        aliases = {len(args): 0}
        args.append(x)
        in_specs.append(pl.BlockSpec(memory_space=pltpu.HBM))
    return pl.pallas_call(
        functools.partial(bulk_kernel, steps, len(aliases)),
        grid=(width // tile,),
        in_specs=in_specs,
        out_specs=[column, pl.BlockSpec((BLOCK, tile), lambda n: (0, n)), pl.BlockSpec((BLOCK, BLOCK), lambda n: (0, 0))],
        out_shape=[
            jax.ShapeDtypeStruct((rows, cols), jnp.bfloat16),
            jax.ShapeDtypeStruct((BLOCK, width), jnp.float32),
            jax.ShapeDtypeStruct((BLOCK, BLOCK), jnp.bfloat16),
        ],
        scratch_shapes=[pltpu.VMEM((2, rows, rows), jnp.bfloat16), pltpu.SemaphoreType.DMA((2 * steps,))],
        input_output_aliases=aliases,
        compiler_params=pltpu.CompilerParams(vmem_limit_bytes=50 << 20),
        cost_estimate=pl.CostEstimate(
            flops=2 * rows * rows * width, bytes_accessed=3 * rows * width * 2, transcendentals=0),
    )(*args)


def finish_kernel(step, start, row, tile, acc_start, l_ref, b_ref, acc_ref, x_in, x_ref, l_buf, b_buf, acc_buf, out_buf, sems):
    del x_in
    rows = pl.ds(step * BLOCK, BLOCK)

    @pl.when(lax.axis_index("row") == row)
    def _():
        l_copy = pltpu.make_async_copy(l_ref, l_buf, sems.at[0])
        b_copy = pltpu.make_async_copy(b_ref, b_buf, sems.at[1])
        acc_copy = pltpu.make_async_copy(acc_ref.at[:, pl.ds(acc_start, b_ref.shape[1])], acc_buf, sems.at[2])
        l_copy.start()
        b_copy.start()
        acc_copy.start()
        l_copy.wait()
        b_copy.wait()
        acc_copy.wait()

        @pl.loop(0, b_ref.shape[1] // tile)
        def _(n):
            columns = pl.ds(pl.multiple_of(n * tile, tile), tile)
            acc = acc_buf[:, columns] + jnp.dot(l_buf[...], b_buf[:, columns], preferred_element_type=jnp.float32)
            out_buf[:, columns] = acc.astype(out_buf.dtype)

        out_copy = pltpu.make_async_copy(out_buf, x_ref.at[rows, pl.ds(start, b_ref.shape[1])], sems.at[3])
        out_copy.start()
        out_copy.wait()


def finish(step, start, row, l_last, piece, acc, acc_start, x):
    width = piece.shape[1]
    return pl.pallas_call(
        functools.partial(finish_kernel, step, start, row, min(width, 512), acc_start),
        in_specs=[pl.BlockSpec(memory_space=pltpu.HBM)] * 4,
        out_specs=pl.BlockSpec(memory_space=pltpu.HBM),
        out_shape=jax.ShapeDtypeStruct(x.shape, x.dtype),
        scratch_shapes=[
            pltpu.VMEM((BLOCK, BLOCK), l_last.dtype),
            pltpu.VMEM((BLOCK, width), piece.dtype),
            pltpu.VMEM((BLOCK, width), acc.dtype),
            pltpu.VMEM((BLOCK, width), x.dtype),
            pltpu.SemaphoreType.DMA((4,)),
        ],
        input_output_aliases={3: 0},
        compiler_params=pltpu.CompilerParams(vmem_limit_bytes=12 << 20),
        cost_estimate=pl.CostEstimate(
            flops=2 * BLOCK * BLOCK * width, bytes_accessed=BLOCK * width * 8, transcendentals=0),
    )(l_last, piece, acc, x)


def last_kernel(step, start, row, l_ref, b_ref, acc_ref, x_in, x_ref, out_buf, sem):
    del x_in

    @pl.when(lax.axis_index("row") == row)
    def _():
        acc = acc_ref[...] + jnp.dot(l_ref[...], b_ref[...], preferred_element_type=jnp.float32)
        out_buf[...] = acc.astype(out_buf.dtype)
        copy = pltpu.make_async_copy(
            out_buf, x_ref.at[pl.ds(step * BLOCK, BLOCK), pl.ds(start, b_ref.shape[1])], sem)
        copy.start()
        copy.wait()


def finish_last(step, start, row, l_last, piece, acc, x):
    width = piece.shape[1]
    return pl.pallas_call(
        functools.partial(last_kernel, step, start, row),
        in_specs=[pl.BlockSpec(memory_space=pltpu.VMEM)] * 3 + [pl.BlockSpec(memory_space=pltpu.HBM)],
        out_specs=pl.BlockSpec(memory_space=pltpu.HBM),
        out_shape=jax.ShapeDtypeStruct(x.shape, x.dtype),
        scratch_shapes=[pltpu.VMEM((BLOCK, width), x.dtype), pltpu.SemaphoreType.DMA],
        input_output_aliases={3: 0},
        compiler_params=pltpu.CompilerParams(vmem_limit_bytes=8 << 20),
        cost_estimate=pl.CostEstimate(
            flops=2 * BLOCK * BLOCK * width, bytes_accessed=BLOCK * width * 8, transcendentals=0),
    )(l_last, piece, acc, x)


def cut_kernel(row, start, b_ref, out_ref, sem):
    @pl.when(lax.axis_index("row") == 0)
    def _():
        copy = pltpu.make_async_copy(b_ref.at[pl.ds(row, BLOCK), pl.ds(start, out_ref.shape[1])], out_ref, sem)
        copy.start()
        copy.wait()


def cut(b, row, start, width):
    return pl.pallas_call(
        functools.partial(cut_kernel, row, start),
        in_specs=[pl.BlockSpec(memory_space=pltpu.HBM)],
        out_specs=pl.BlockSpec(memory_space=pl.ANY),
        out_shape=jax.ShapeDtypeStruct((BLOCK, width), b.dtype),
        scratch_shapes=[pltpu.SemaphoreType.DMA],
        compiler_params=pltpu.CompilerParams(vmem_limit_bytes=48 << 20),
        cost_estimate=pl.CostEstimate(flops=2 * BLOCK * width, bytes_accessed=BLOCK * width * 4, transcendentals=0),
    )(b)


def keep_kernel(row, piece_ref, out_ref, sem):
    @pl.when(lax.axis_index("row") == row)
    def _():
        copy = pltpu.make_async_copy(piece_ref, out_ref, sem)
        copy.start()
        copy.wait()


def keep(row, piece):
    return pl.pallas_call(
        functools.partial(keep_kernel, row),
        in_specs=[pl.BlockSpec(memory_space=pltpu.VMEM)],
        out_specs=pl.BlockSpec(memory_space=pltpu.HBM),
        out_shape=jax.ShapeDtypeStruct(piece.shape, piece.dtype),
        scratch_shapes=[pltpu.SemaphoreType.DMA],
        compiler_params=pltpu.CompilerParams(vmem_limit_bytes=1 << 20),
        cost_estimate=pl.CostEstimate(flops=2 * piece.size, bytes_accessed=4 * piece.size, transcendentals=0),
    )(piece)


def cut_many_kernel(places, b_ref, *refs):
    count = len(places)
    out_refs, bufs, sems = refs[:count], refs[count:2 * count], refs[2 * count]
    fetches = [
        pltpu.make_async_copy(b_ref.at[pl.ds(row, BLOCK), pl.ds(start, width)], bufs[i], sems.at[0, i])
        for i, (row, start, width) in enumerate(places)]
    stores = [pltpu.make_async_copy(bufs[i], out_refs[i], sems.at[1, i]) for i in range(count)]
    for fetch in fetches:
        fetch.start()
    for fetch, store in zip(fetches, stores):
        fetch.wait()
        store.start()
    for store in stores:
        store.wait()


def cut_many(b, places):
    size = sum(width for _, _, width in places) * BLOCK
    return pl.pallas_call(
        functools.partial(cut_many_kernel, places),
        in_specs=[pl.BlockSpec(memory_space=pltpu.HBM)],
        out_specs=[pl.BlockSpec(memory_space=pltpu.HBM)] * len(places),
        out_shape=[jax.ShapeDtypeStruct((BLOCK, width), b.dtype) for _, _, width in places],
        scratch_shapes=[pltpu.VMEM((BLOCK, width), b.dtype) for _, _, width in places]
        + [pltpu.SemaphoreType.DMA((2, len(places)))],
        compiler_params=pltpu.CompilerParams(vmem_limit_bytes=48 << 20),
        cost_estimate=pl.CostEstimate(flops=2 * size, bytes_accessed=4 * size, transcendentals=0),
    )(b)


def solution(mesh):
    grid_rows = mesh.shape["row"]
    grid_cols = mesh.shape["col"]
    swap_row = [(r, r ^ 1) for r in range(grid_rows)]
    down_row = [(r, r + 1) for r in range(grid_rows - 1)]

    def local_trmm(tri_loc, rhs_loc):
        rows, cols = rhs_loc.shape
        steps = rows // BLOCK
        final = steps - 1
        half = cols // 2
        first = cols // 16

        order = [(final, cols - first, first)]
        order += [(j, h * half, half) for j in range(final) for h in range(2)]
        tail = [(0, half), (half, cols // 4), (half + cols // 4, cols // 8), (cols - 2 * first, first)]
        order += [(final, off, w) for off, w in tail]

        got = {}

        def send(i, piece):
            j, off, _ = order[i]
            got[j, off] = lax.ppermute(piece, "row", down_row if i and j == final else swap_row)

        places = [(j * BLOCK, off, w) for j, off, w in order]
        piece = cut(rhs_loc, *places[0])
        send(0, piece)
        piece, = cut_many(rhs_loc, places[1:2])
        send(1, piece)
        pieces = cut_many(rhs_loc, places[2:-1])
        for i, piece in enumerate(pieces):
            send(2 + i, piece)
        got[final, cols - first] = keep(grid_rows - 1, got[final, cols - first])
        l_core, l_chip, l_both = (
            lax.ppermute(tri_loc, "col", [(c, c ^ d) for c in range(grid_cols)]) for d in (1, 2, 3))
        l_parts = [tri_loc, l_core, l_chip, l_both]

        x, acc = None, [None, None]
        for h in range(2):
            x, acc[h], l_last = bulk(h * half, 512, l_parts, rhs_loc, [got[k, h * half] for k in range(final)], x)
        off, w = tail[-1]
        acc_last = acc[1][:, off - half:off - half + w]
        source, acc[1] = lax.optimization_barrier((rhs_loc, acc[1]))
        send(len(order) - 1, source[final * BLOCK:, off:off + w])
        for off, w in [(cols - first, first), *tail[:-1]]:
            h = off // half
            x = finish(final, off, grid_rows - 1, l_last, got[final, off], acc[h], off - h * half, x)
        off, w = tail[-1]
        return finish_last(final, off, grid_rows - 1, l_last, got[final, off], acc_last, x)

    part_spec = P(("batch", "row"), "col")
    return jax.shard_map(local_trmm, mesh=mesh, in_specs=(part_spec, part_spec), out_specs=part_spec, check_vma=False)
```

```python
import functools

import jax
import jax.numpy as jnp
from jax import lax
from jax.experimental import pallas as pl
from jax.experimental.pallas import tpu as pltpu
from jax.sharding import PartitionSpec as P


BLOCK = 256


def bulk_kernel(steps, aliased, early, *refs):
    l_refs, bo_ref, rem_refs = refs[:4], refs[4], refs[5:4 + steps]
    x_ref, acc_ref, last_ref, l_buf, sems = refs[4 + steps + aliased + early:]

    @pl.when(pl.program_id(0) == 0)
    def _():
        row, col = lax.axis_index("row"), lax.axis_index("col")
        copies = []
        for d in range(4):
            chip, core = (col // 2 + d // 2) % 2, (col + d) % 2
            side = (core + row) % 2
            for j in range(steps // 2):
                place = pl.multiple_of((2 * j + chip) * BLOCK, BLOCK)
                copies.append(pltpu.make_async_copy(
                    l_refs[d].at[:, pl.ds(j * BLOCK, BLOCK)], l_buf.at[side, :, pl.ds(place, BLOCK)], sems.at[len(copies)]))
        for copy in copies:
            copy.start()
        for copy in copies:
            copy.wait()
        last_ref[...] = l_buf[1, (steps - 1) * BLOCK:, (steps - 1) * BLOCK:]

    for step in range(steps):
        rows = slice(step * BLOCK, (step + 1) * BLOCK)
        depth = (step + 1) * BLOCK
        acc = jnp.dot(l_buf[0, rows, :depth], bo_ref[:depth, :], preferred_element_type=jnp.float32)
        for j in range(min(step + 1, steps - 1)):
            columns = slice(j * BLOCK, (j + 1) * BLOCK)
            acc += jnp.dot(l_buf[1, rows, columns], rem_refs[j][...], preferred_element_type=jnp.float32)
        x_ref[rows, :] = acc.astype(x_ref.dtype)
    acc_ref[...] = acc

    if early:
        early_ref = refs[4 + steps]

        @pl.when((pl.program_id(0) == pl.num_programs(0) - 1) & (lax.axis_index("row") == 1))
        def _():
            done = acc_ref[...] + jnp.dot(last_ref[...], early_ref[...], preferred_element_type=jnp.float32)
            x_ref[(steps - 1) * BLOCK:, :] = done.astype(x_ref.dtype)


def bulk(start, tile, l_parts, b_own, pieces, early, x):
    rows, cols = b_own.shape
    steps = rows // BLOCK
    width = pieces[0].shape[1]
    base = start // tile
    column = pl.BlockSpec((rows, tile), lambda n: (0, base + n))
    in_specs = [pl.BlockSpec(memory_space=pltpu.HBM)] * 4 + [column]
    in_specs += [pl.BlockSpec((BLOCK, tile), lambda n: (0, n))] * (steps - 1)
    args = [*l_parts, b_own, *pieces]
    if early is not None:
        args.append(early)
        in_specs.append(pl.BlockSpec((BLOCK, tile), lambda n: (0, 0)))
    aliases = {}
    if x is not None:
        aliases = {len(args): 0}
        args.append(x)
        in_specs.append(pl.BlockSpec(memory_space=pltpu.HBM))
    return pl.pallas_call(
        functools.partial(bulk_kernel, steps, len(aliases), int(early is not None)),
        grid=(width // tile,),
        in_specs=in_specs,
        out_specs=[column, pl.BlockSpec((BLOCK, tile), lambda n: (0, n)), pl.BlockSpec((BLOCK, BLOCK), lambda n: (0, 0))],
        out_shape=[
            jax.ShapeDtypeStruct((rows, cols), jnp.bfloat16),
            jax.ShapeDtypeStruct((BLOCK, width), jnp.float32),
            jax.ShapeDtypeStruct((BLOCK, BLOCK), jnp.bfloat16),
        ],
        scratch_shapes=[pltpu.VMEM((2, rows, rows), jnp.bfloat16), pltpu.SemaphoreType.DMA((2 * steps,))],
        input_output_aliases=aliases,
        compiler_params=pltpu.CompilerParams(vmem_limit_bytes=50 << 20),
        cost_estimate=pl.CostEstimate(
            flops=2 * rows * rows * width, bytes_accessed=3 * rows * width * 2, transcendentals=0),
    )(*args)


def finish_kernel(step, start, row, tile, acc_start, l_ref, b_ref, acc_ref, x_in, x_ref, l_buf, b_buf, acc_buf, out_buf, sems):
    del x_in
    rows = pl.ds(step * BLOCK, BLOCK)

    @pl.when(lax.axis_index("row") == row)
    def _():
        l_copy = pltpu.make_async_copy(l_ref, l_buf, sems.at[0])
        b_copy = pltpu.make_async_copy(b_ref, b_buf, sems.at[1])
        acc_copy = pltpu.make_async_copy(acc_ref.at[:, pl.ds(acc_start, b_ref.shape[1])], acc_buf, sems.at[2])
        l_copy.start()
        b_copy.start()
        acc_copy.start()
        l_copy.wait()
        b_copy.wait()
        acc_copy.wait()

        @pl.loop(0, b_ref.shape[1] // tile)
        def _(n):
            columns = pl.ds(pl.multiple_of(n * tile, tile), tile)
            acc = acc_buf[:, columns] + jnp.dot(l_buf[...], b_buf[:, columns], preferred_element_type=jnp.float32)
            out_buf[:, columns] = acc.astype(out_buf.dtype)

        out_copy = pltpu.make_async_copy(out_buf, x_ref.at[rows, pl.ds(start, b_ref.shape[1])], sems.at[3])
        out_copy.start()
        out_copy.wait()


def finish(step, start, row, l_last, piece, acc, acc_start, x):
    width = piece.shape[1]
    return pl.pallas_call(
        functools.partial(finish_kernel, step, start, row, min(width, 512), acc_start),
        in_specs=[pl.BlockSpec(memory_space=pltpu.HBM)] * 4,
        out_specs=pl.BlockSpec(memory_space=pltpu.HBM),
        out_shape=jax.ShapeDtypeStruct(x.shape, x.dtype),
        scratch_shapes=[
            pltpu.VMEM((BLOCK, BLOCK), l_last.dtype),
            pltpu.VMEM((BLOCK, width), piece.dtype),
            pltpu.VMEM((BLOCK, width), acc.dtype),
            pltpu.VMEM((BLOCK, width), x.dtype),
            pltpu.SemaphoreType.DMA((4,)),
        ],
        input_output_aliases={3: 0},
        compiler_params=pltpu.CompilerParams(vmem_limit_bytes=12 << 20),
        cost_estimate=pl.CostEstimate(
            flops=2 * BLOCK * BLOCK * width, bytes_accessed=BLOCK * width * 8, transcendentals=0),
    )(l_last, piece, acc, x)


def last_kernel(step, start, row, l_ref, b_ref, acc_ref, x_in, x_ref, out_buf, sem):
    del x_in

    @pl.when(lax.axis_index("row") == row)
    def _():
        acc = acc_ref[...] + jnp.dot(l_ref[...], b_ref[...], preferred_element_type=jnp.float32)
        out_buf[...] = acc.astype(out_buf.dtype)
        copy = pltpu.make_async_copy(
            out_buf, x_ref.at[pl.ds(step * BLOCK, BLOCK), pl.ds(start, b_ref.shape[1])], sem)
        copy.start()
        copy.wait()


def finish_last(step, start, row, l_last, piece, acc, x):
    width = piece.shape[1]
    return pl.pallas_call(
        functools.partial(last_kernel, step, start, row),
        in_specs=[pl.BlockSpec(memory_space=pltpu.VMEM)] * 3 + [pl.BlockSpec(memory_space=pltpu.HBM)],
        out_specs=pl.BlockSpec(memory_space=pltpu.HBM),
        out_shape=jax.ShapeDtypeStruct(x.shape, x.dtype),
        scratch_shapes=[pltpu.VMEM((BLOCK, width), x.dtype), pltpu.SemaphoreType.DMA],
        input_output_aliases={3: 0},
        compiler_params=pltpu.CompilerParams(vmem_limit_bytes=8 << 20),
        cost_estimate=pl.CostEstimate(
            flops=2 * BLOCK * BLOCK * width, bytes_accessed=BLOCK * width * 8, transcendentals=0),
    )(l_last, piece, acc, x)


def cut_kernel(row, start, b_ref, out_ref, sem):
    @pl.when(lax.axis_index("row") == 0)
    def _():
        copy = pltpu.make_async_copy(b_ref.at[pl.ds(row, BLOCK), pl.ds(start, out_ref.shape[1])], out_ref, sem)
        copy.start()
        copy.wait()


def cut(b, row, start, width):
    return pl.pallas_call(
        functools.partial(cut_kernel, row, start),
        in_specs=[pl.BlockSpec(memory_space=pltpu.HBM)],
        out_specs=pl.BlockSpec(memory_space=pl.ANY),
        out_shape=jax.ShapeDtypeStruct((BLOCK, width), b.dtype),
        scratch_shapes=[pltpu.SemaphoreType.DMA],
        compiler_params=pltpu.CompilerParams(vmem_limit_bytes=48 << 20),
        cost_estimate=pl.CostEstimate(flops=2 * BLOCK * width, bytes_accessed=BLOCK * width * 4, transcendentals=0),
    )(b)


def keep_kernel(row, piece_ref, out_ref, sem):
    @pl.when(lax.axis_index("row") == row)
    def _():
        copy = pltpu.make_async_copy(piece_ref, out_ref, sem)
        copy.start()
        copy.wait()


def keep(row, piece):
    return pl.pallas_call(
        functools.partial(keep_kernel, row),
        in_specs=[pl.BlockSpec(memory_space=pltpu.VMEM)],
        out_specs=pl.BlockSpec(memory_space=pltpu.HBM),
        out_shape=jax.ShapeDtypeStruct(piece.shape, piece.dtype),
        scratch_shapes=[pltpu.SemaphoreType.DMA],
        compiler_params=pltpu.CompilerParams(vmem_limit_bytes=1 << 20),
        cost_estimate=pl.CostEstimate(flops=2 * piece.size, bytes_accessed=4 * piece.size, transcendentals=0),
    )(piece)


def cut_many_kernel(places, b_ref, *refs):
    count = len(places)
    out_refs, bufs, sems = refs[:count], refs[count:2 * count], refs[2 * count]
    fetches = [
        pltpu.make_async_copy(b_ref.at[pl.ds(row, BLOCK), pl.ds(start, width)], bufs[i], sems.at[0, i])
        for i, (row, start, width) in enumerate(places)]
    stores = [pltpu.make_async_copy(bufs[i], out_refs[i], sems.at[1, i]) for i in range(count)]
    for fetch in fetches:
        fetch.start()
    for fetch, store in zip(fetches, stores):
        fetch.wait()
        store.start()
    for store in stores:
        store.wait()


def cut_many(b, places):
    size = sum(width for _, _, width in places) * BLOCK
    return pl.pallas_call(
        functools.partial(cut_many_kernel, places),
        in_specs=[pl.BlockSpec(memory_space=pltpu.HBM)],
        out_specs=[pl.BlockSpec(memory_space=pltpu.HBM)] * len(places),
        out_shape=[jax.ShapeDtypeStruct((BLOCK, width), b.dtype) for _, _, width in places],
        scratch_shapes=[pltpu.VMEM((BLOCK, width), b.dtype) for _, _, width in places]
        + [pltpu.SemaphoreType.DMA((2, len(places)))],
        compiler_params=pltpu.CompilerParams(vmem_limit_bytes=48 << 20),
        cost_estimate=pl.CostEstimate(flops=2 * size, bytes_accessed=4 * size, transcendentals=0),
    )(b)


def solution(mesh):
    grid_rows = mesh.shape["row"]
    grid_cols = mesh.shape["col"]
    swap_row = [(r, r ^ 1) for r in range(grid_rows)]
    down_row = [(r, r + 1) for r in range(grid_rows - 1)]

    def local_trmm(tri_loc, rhs_loc):
        rows, cols = rhs_loc.shape
        steps = rows // BLOCK
        final = steps - 1
        half = cols // 2
        first = cols // 16

        order = [(final, cols - first, first)]
        order += [(j, h * half, half) for j in range(final) for h in range(2)]
        tail = [(0, half), (half, cols // 4), (half + cols // 4, cols // 8), (cols - 2 * first, first)]
        order += [(final, off, w) for off, w in tail]

        got = {}

        def send(i, piece):
            j, off, _ = order[i]
            got[j, off] = lax.ppermute(piece, "row", down_row if i and j == final else swap_row)

        places = [(j * BLOCK, off, w) for j, off, w in order]
        piece = cut(rhs_loc, *places[0])
        send(0, piece)
        piece, = cut_many(rhs_loc, places[1:2])
        send(1, piece)
        pieces = cut_many(rhs_loc, places[2:-1])
        for i, piece in enumerate(pieces):
            send(2 + i, piece)
        got[final, cols - first] = keep(grid_rows - 1, got[final, cols - first])
        l_core, l_chip, l_both = (
            lax.ppermute(tri_loc, "col", [(c, c ^ d) for c in range(grid_cols)]) for d in (1, 2, 3))
        l_parts = [tri_loc, l_core, l_chip, l_both]

        x, acc = None, [None, None]
        for h in range(2):
            early = got[final, cols - first] if h == 1 else None
            x, acc[h], l_last = bulk(h * half, first, l_parts, rhs_loc, [got[k, h * half] for k in range(final)], early, x)
        off, w = tail[-1]
        acc_last = acc[1][:, off - half:off - half + w]
        source, acc[1] = lax.optimization_barrier((rhs_loc, acc[1]))
        send(len(order) - 1, source[final * BLOCK:, off:off + w])
        for off, w in tail[:-1]:
            h = off // half
            x = finish(final, off, grid_rows - 1, l_last, got[final, off], acc[h], off - h * half, x)
        off, w = tail[-1]
        return finish_last(final, off, grid_rows - 1, l_last, got[final, off], acc_last, x)

    part_spec = P(("batch", "row"), "col")
    return jax.shard_map(local_trmm, mesh=mesh, in_specs=(part_spec, part_spec), out_specs=part_spec, check_vma=False)
```

```python
import functools

import jax
import jax.numpy as jnp
from jax import lax
from jax.experimental import pallas as pl
from jax.experimental.pallas import tpu as pltpu
from jax.sharding import PartitionSpec as P


BLOCK = 256


def bulk_kernel(steps, *refs):
    l_refs, bo_ref, early_ref = refs[:4], refs[4], refs[5]
    rem_refs = [refs[6 + h * (steps - 1):6 + (h + 1) * (steps - 1)] for h in range(2)]
    x_ref, acc_ref, last_ref, l_buf, sems = refs[4 + 2 * steps:]
    tile_id, tiles = pl.program_id(0), pl.num_programs(0)

    @pl.when(pl.program_id(0) == 0)
    def _():
        row, col = lax.axis_index("row"), lax.axis_index("col")
        copies = []
        for d in range(4):
            chip, core = (col // 2 + d // 2) % 2, (col + d) % 2
            side = (core + row) % 2
            for j in range(steps // 2):
                place = pl.multiple_of((2 * j + chip) * BLOCK, BLOCK)
                copies.append(pltpu.make_async_copy(
                    l_refs[d].at[:, pl.ds(j * BLOCK, BLOCK)], l_buf.at[side, :, pl.ds(place, BLOCK)], sems.at[len(copies)]))
        for copy in copies:
            copy.start()
        for copy in copies:
            copy.wait()
        last_ref[...] = l_buf[1, (steps - 1) * BLOCK:, (steps - 1) * BLOCK:]

    def multiply(received):
        for step in range(steps):
            rows = slice(step * BLOCK, (step + 1) * BLOCK)
            depth = (step + 1) * BLOCK
            acc = jnp.dot(l_buf[0, rows, :depth], bo_ref[:depth, :], preferred_element_type=jnp.float32)
            for j in range(min(step + 1, steps - 1)):
                columns = slice(j * BLOCK, (j + 1) * BLOCK)
                acc += jnp.dot(l_buf[1, rows, columns], received[j][...], preferred_element_type=jnp.float32)
            x_ref[rows, :] = acc.astype(x_ref.dtype)
        acc_ref[...] = acc

    for h in range(2):
        pl.when(tile_id // (tiles // 2) == h)(functools.partial(multiply, rem_refs[h]))

    @pl.when((tile_id == tiles - 1) & (lax.axis_index("row") == 1))
    def _():
        done = acc_ref[...] + jnp.dot(last_ref[...], early_ref[...], preferred_element_type=jnp.float32)
        x_ref[(steps - 1) * BLOCK:, :] = done.astype(x_ref.dtype)


def bulk(tile, l_parts, b_own, early, halves):
    rows, cols = b_own.shape
    steps = rows // BLOCK
    tiles = cols // tile
    column = pl.BlockSpec((rows, tile), lambda n: (0, n))
    in_specs = [pl.BlockSpec(memory_space=pltpu.HBM)] * 4 + [column, pl.BlockSpec((BLOCK, tile), lambda n: (0, 0))]
    in_specs += [pl.BlockSpec((BLOCK, tile), lambda n: (0, jnp.minimum(n, tiles // 2 - 1)))] * (steps - 1)
    in_specs += [pl.BlockSpec((BLOCK, tile), lambda n: (0, jnp.maximum(n - tiles // 2, 0)))] * (steps - 1)
    return pl.pallas_call(
        functools.partial(bulk_kernel, steps),
        grid=(tiles,),
        in_specs=in_specs,
        out_specs=[column, pl.BlockSpec((BLOCK, tile), lambda n: (0, n)), pl.BlockSpec((BLOCK, BLOCK), lambda n: (0, 0))],
        out_shape=[
            jax.ShapeDtypeStruct((rows, cols), jnp.bfloat16),
            jax.ShapeDtypeStruct((BLOCK, cols), jnp.float32),
            jax.ShapeDtypeStruct((BLOCK, BLOCK), jnp.bfloat16),
        ],
        scratch_shapes=[pltpu.VMEM((2, rows, rows), jnp.bfloat16), pltpu.SemaphoreType.DMA((2 * steps,))],
        compiler_params=pltpu.CompilerParams(vmem_limit_bytes=50 << 20),
        cost_estimate=pl.CostEstimate(
            flops=2 * rows * rows * cols, bytes_accessed=3 * rows * cols * 2, transcendentals=0),
    )(*l_parts, b_own, early, *halves[0], *halves[1])


def finish_kernel(step, start, row, tile, acc_start, l_ref, b_ref, acc_ref, x_in, x_ref, l_buf, b_buf, acc_buf, out_buf, sems):
    del x_in
    rows = pl.ds(step * BLOCK, BLOCK)

    @pl.when(lax.axis_index("row") == row)
    def _():
        l_copy = pltpu.make_async_copy(l_ref, l_buf, sems.at[0])
        b_copy = pltpu.make_async_copy(b_ref, b_buf, sems.at[1])
        acc_copy = pltpu.make_async_copy(acc_ref.at[:, pl.ds(acc_start, b_ref.shape[1])], acc_buf, sems.at[2])
        l_copy.start()
        b_copy.start()
        acc_copy.start()
        l_copy.wait()
        b_copy.wait()
        acc_copy.wait()

        @pl.loop(0, b_ref.shape[1] // tile)
        def _(n):
            columns = pl.ds(pl.multiple_of(n * tile, tile), tile)
            acc = acc_buf[:, columns] + jnp.dot(l_buf[...], b_buf[:, columns], preferred_element_type=jnp.float32)
            out_buf[:, columns] = acc.astype(out_buf.dtype)

        out_copy = pltpu.make_async_copy(out_buf, x_ref.at[rows, pl.ds(start, b_ref.shape[1])], sems.at[3])
        out_copy.start()
        out_copy.wait()


def finish(step, start, row, l_last, piece, acc, acc_start, x):
    width = piece.shape[1]
    return pl.pallas_call(
        functools.partial(finish_kernel, step, start, row, min(width, 512), acc_start),
        in_specs=[pl.BlockSpec(memory_space=pltpu.HBM)] * 4,
        out_specs=pl.BlockSpec(memory_space=pltpu.HBM),
        out_shape=jax.ShapeDtypeStruct(x.shape, x.dtype),
        scratch_shapes=[
            pltpu.VMEM((BLOCK, BLOCK), l_last.dtype),
            pltpu.VMEM((BLOCK, width), piece.dtype),
            pltpu.VMEM((BLOCK, width), acc.dtype),
            pltpu.VMEM((BLOCK, width), x.dtype),
            pltpu.SemaphoreType.DMA((4,)),
        ],
        input_output_aliases={3: 0},
        compiler_params=pltpu.CompilerParams(vmem_limit_bytes=12 << 20),
        cost_estimate=pl.CostEstimate(
            flops=2 * BLOCK * BLOCK * width, bytes_accessed=BLOCK * width * 8, transcendentals=0),
    )(l_last, piece, acc, x)


def last_kernel(step, start, row, l_ref, b_ref, acc_ref, x_in, x_ref, out_buf, sem):
    del x_in

    @pl.when(lax.axis_index("row") == row)
    def _():
        acc = acc_ref[...] + jnp.dot(l_ref[...], b_ref[...], preferred_element_type=jnp.float32)
        out_buf[...] = acc.astype(out_buf.dtype)
        copy = pltpu.make_async_copy(
            out_buf, x_ref.at[pl.ds(step * BLOCK, BLOCK), pl.ds(start, b_ref.shape[1])], sem)
        copy.start()
        copy.wait()


def finish_last(step, start, row, l_last, piece, acc, x):
    width = piece.shape[1]
    return pl.pallas_call(
        functools.partial(last_kernel, step, start, row),
        in_specs=[pl.BlockSpec(memory_space=pltpu.VMEM)] * 3 + [pl.BlockSpec(memory_space=pltpu.HBM)],
        out_specs=pl.BlockSpec(memory_space=pltpu.HBM),
        out_shape=jax.ShapeDtypeStruct(x.shape, x.dtype),
        scratch_shapes=[pltpu.VMEM((BLOCK, width), x.dtype), pltpu.SemaphoreType.DMA],
        input_output_aliases={3: 0},
        compiler_params=pltpu.CompilerParams(vmem_limit_bytes=8 << 20),
        cost_estimate=pl.CostEstimate(
            flops=2 * BLOCK * BLOCK * width, bytes_accessed=BLOCK * width * 8, transcendentals=0),
    )(l_last, piece, acc, x)


def cut_kernel(row, start, b_ref, out_ref, sem):
    @pl.when(lax.axis_index("row") == 0)
    def _():
        copy = pltpu.make_async_copy(b_ref.at[pl.ds(row, BLOCK), pl.ds(start, out_ref.shape[1])], out_ref, sem)
        copy.start()
        copy.wait()


def cut(b, row, start, width):
    return pl.pallas_call(
        functools.partial(cut_kernel, row, start),
        in_specs=[pl.BlockSpec(memory_space=pltpu.HBM)],
        out_specs=pl.BlockSpec(memory_space=pl.ANY),
        out_shape=jax.ShapeDtypeStruct((BLOCK, width), b.dtype),
        scratch_shapes=[pltpu.SemaphoreType.DMA],
        compiler_params=pltpu.CompilerParams(vmem_limit_bytes=48 << 20),
        cost_estimate=pl.CostEstimate(flops=2 * BLOCK * width, bytes_accessed=BLOCK * width * 4, transcendentals=0),
    )(b)


def keep_kernel(row, piece_ref, out_ref, sem):
    @pl.when(lax.axis_index("row") == row)
    def _():
        copy = pltpu.make_async_copy(piece_ref, out_ref, sem)
        copy.start()
        copy.wait()


def keep(row, piece):
    return pl.pallas_call(
        functools.partial(keep_kernel, row),
        in_specs=[pl.BlockSpec(memory_space=pltpu.VMEM)],
        out_specs=pl.BlockSpec(memory_space=pltpu.HBM),
        out_shape=jax.ShapeDtypeStruct(piece.shape, piece.dtype),
        scratch_shapes=[pltpu.SemaphoreType.DMA],
        compiler_params=pltpu.CompilerParams(vmem_limit_bytes=1 << 20),
        cost_estimate=pl.CostEstimate(flops=2 * piece.size, bytes_accessed=4 * piece.size, transcendentals=0),
    )(piece)


def cut_rest_kernel(places, b_ref, *refs):
    count = len(places)
    out_refs, (head, body, fetch_sems, store_sems) = refs[:count], refs[count:]
    first_row, first_start, first_width = places[0]
    fetches = [pltpu.make_async_copy(b_ref.at[pl.ds(first_row, BLOCK), pl.ds(first_start, first_width)], head, fetch_sems.at[0])]
    stores = [pltpu.make_async_copy(head, out_refs[0], store_sems.at[0])]
    if count > 1:
        fetches.append(pltpu.make_async_copy(b_ref.at[pl.ds(BLOCK, body.shape[0])], body, fetch_sems.at[1]))
        for i, (row, start, width) in list(enumerate(places))[1:]:
            piece = body.at[pl.ds(row - BLOCK, BLOCK), pl.ds(start, width)]
            stores.append(pltpu.make_async_copy(piece, out_refs[i], store_sems.at[i]))
    for fetch in fetches:
        fetch.start()
    fetches[0].wait()
    stores[0].start()
    if count > 1:
        fetches[1].wait()
    for store in stores[1:]:
        store.start()
    for store in stores:
        store.wait()


def cut_rest(b, places):
    size = sum(width for _, _, width in places) * BLOCK
    body = (b.shape[0] - BLOCK, b.shape[1]) if len(places) > 1 else (BLOCK, BLOCK)
    return pl.pallas_call(
        functools.partial(cut_rest_kernel, places),
        in_specs=[pl.BlockSpec(memory_space=pltpu.HBM)],
        out_specs=[pl.BlockSpec(memory_space=pltpu.HBM)] * len(places),
        out_shape=[jax.ShapeDtypeStruct((BLOCK, width), b.dtype) for _, _, width in places],
        scratch_shapes=[
            pltpu.VMEM((BLOCK, places[0][2]), b.dtype),
            pltpu.VMEM(body, b.dtype),
            pltpu.SemaphoreType.DMA((2,)),
            pltpu.SemaphoreType.DMA((len(places),)),
        ],
        compiler_params=pltpu.CompilerParams(vmem_limit_bytes=48 << 20),
        cost_estimate=pl.CostEstimate(flops=2 * size, bytes_accessed=4 * size, transcendentals=0),
    )(b)


def solution(mesh):
    grid_rows = mesh.shape["row"]
    grid_cols = mesh.shape["col"]
    swap_row = [(r, r ^ 1) for r in range(grid_rows)]
    down_row = [(r, r + 1) for r in range(grid_rows - 1)]

    def local_trmm(tri_loc, rhs_loc):
        rows, cols = rhs_loc.shape
        steps = rows // BLOCK
        final = steps - 1
        half = cols // 2
        first = cols // 16

        order = [(final, cols - first, first)]
        order += [(j, h * half, half) for j in range(final) for h in range(2)]
        tail = [(0, half), (half, cols // 4), (half + cols // 4, cols // 8), (cols - 2 * first, first)]
        order += [(final, off, w) for off, w in tail]

        got = {}

        def send(i, piece):
            j, off, _ = order[i]
            got[j, off] = lax.ppermute(piece, "row", down_row if i and j == final else swap_row)

        places = [(j * BLOCK, off, w) for j, off, w in order]
        piece = cut(rhs_loc, *places[0])
        send(0, piece)
        piece, = cut_rest(rhs_loc, places[1:2])
        send(1, piece)
        pieces = cut_rest(rhs_loc, places[2:-1])
        for i, piece in enumerate(pieces):
            send(2 + i, piece)
        got[final, cols - first] = keep(grid_rows - 1, got[final, cols - first])
        l_core, l_chip, l_both = (
            lax.ppermute(tri_loc, "col", [(c, c ^ d) for c in range(grid_cols)]) for d in (1, 2, 3))
        l_parts = [tri_loc, l_core, l_chip, l_both]

        halves = [[got[k, h * half] for k in range(final)] for h in range(2)]
        x, acc, l_last = bulk(first, l_parts, rhs_loc, got[final, cols - first], halves)
        off, w = tail[-1]
        acc_last = acc[:, off:off + w]
        source, acc = lax.optimization_barrier((rhs_loc, acc))
        send(len(order) - 1, source[final * BLOCK:, off:off + w])
        for off, w in tail[:-1]:
            x = finish(final, off, grid_rows - 1, l_last, got[final, off], acc, off, x)
        off, w = tail[-1]
        return finish_last(final, off, grid_rows - 1, l_last, got[final, off], acc_last, x)

    part_spec = P(("batch", "row"), "col")
    return jax.shard_map(local_trmm, mesh=mesh, in_specs=(part_spec, part_spec), out_specs=part_spec, check_vma=False)
```

```python
import functools

import jax
import jax.numpy as jnp
from jax import lax
from jax.experimental import pallas as pl
from jax.experimental.pallas import tpu as pltpu
from jax.sharding import PartitionSpec as P


BLOCK = 256


def bulk_kernel(steps, aliased, early, *refs):
    l_refs, bo_ref, rem_refs = refs[:4], refs[4], refs[5:4 + steps]
    x_ref, acc_ref, last_ref, l_buf, sems = refs[4 + steps + aliased + early:]

    @pl.when(pl.program_id(0) == 0)
    def _():
        row, col = lax.axis_index("row"), lax.axis_index("col")
        copies = []
        for d in range(4):
            chip, core = (col // 2 + d // 2) % 2, (col + d) % 2
            side = (core + row) % 2
            for j in range(steps // 2):
                place = pl.multiple_of((2 * j + chip) * BLOCK, BLOCK)
                copies.append(pltpu.make_async_copy(
                    l_refs[d].at[:, pl.ds(j * BLOCK, BLOCK)], l_buf.at[side, :, pl.ds(place, BLOCK)], sems.at[len(copies)]))
        for copy in copies:
            copy.start()
        for copy in copies:
            copy.wait()
        last_ref[...] = l_buf[1, (steps - 1) * BLOCK:, (steps - 1) * BLOCK:]

    for step in range(steps):
        rows = slice(step * BLOCK, (step + 1) * BLOCK)
        depth = (step + 1) * BLOCK
        acc = jnp.dot(l_buf[0, rows, :depth], bo_ref[:depth, :], preferred_element_type=jnp.float32)
        for j in range(min(step + 1, steps - 1)):
            columns = slice(j * BLOCK, (j + 1) * BLOCK)
            acc += jnp.dot(l_buf[1, rows, columns], rem_refs[j][...], preferred_element_type=jnp.float32)
        x_ref[rows, :] = acc.astype(x_ref.dtype)
    acc_ref[...] = acc

    if early:
        early_ref = refs[4 + steps]

        @pl.when((pl.program_id(0) == pl.num_programs(0) - 1) & (lax.axis_index("row") == 1))
        def _():
            done = acc_ref[...] + jnp.dot(last_ref[...], early_ref[...], preferred_element_type=jnp.float32)
            x_ref[(steps - 1) * BLOCK:, :] = done.astype(x_ref.dtype)


def bulk(start, tile, l_parts, b_own, pieces, early, x):
    rows, cols = b_own.shape
    steps = rows // BLOCK
    width = pieces[0].shape[1]
    base = start // tile
    column = pl.BlockSpec((rows, tile), lambda n: (0, base + n))
    in_specs = [pl.BlockSpec(memory_space=pltpu.HBM)] * 4 + [column]
    in_specs += [pl.BlockSpec((BLOCK, tile), lambda n: (0, n))] * (steps - 1)
    args = [*l_parts, b_own, *pieces]
    if early is not None:
        args.append(early)
        in_specs.append(pl.BlockSpec((BLOCK, tile), lambda n: (0, 0)))
    aliases = {}
    if x is not None:
        aliases = {len(args): 0}
        args.append(x)
        in_specs.append(pl.BlockSpec(memory_space=pltpu.HBM))
    return pl.pallas_call(
        functools.partial(bulk_kernel, steps, len(aliases), int(early is not None)),
        grid=(width // tile,),
        in_specs=in_specs,
        out_specs=[column, pl.BlockSpec((BLOCK, tile), lambda n: (0, n)), pl.BlockSpec((BLOCK, BLOCK), lambda n: (0, 0))],
        out_shape=[
            jax.ShapeDtypeStruct((rows, cols), jnp.bfloat16),
            jax.ShapeDtypeStruct((BLOCK, width), jnp.float32),
            jax.ShapeDtypeStruct((BLOCK, BLOCK), jnp.bfloat16),
        ],
        scratch_shapes=[pltpu.VMEM((2, rows, rows), jnp.bfloat16), pltpu.SemaphoreType.DMA((2 * steps,))],
        input_output_aliases=aliases,
        compiler_params=pltpu.CompilerParams(vmem_limit_bytes=50 << 20),
        cost_estimate=pl.CostEstimate(
            flops=2 * rows * rows * width, bytes_accessed=3 * rows * width * 2, transcendentals=0),
    )(*args)


def finish_kernel(step, start, row, tile, acc_start, l_ref, b_ref, acc_ref, x_in, x_ref, l_buf, b_buf, acc_buf, out_buf, sems):
    del x_in
    rows = pl.ds(step * BLOCK, BLOCK)

    @pl.when(lax.axis_index("row") == row)
    def _():
        l_copy = pltpu.make_async_copy(l_ref, l_buf, sems.at[0])
        b_copy = pltpu.make_async_copy(b_ref, b_buf, sems.at[1])
        acc_copy = pltpu.make_async_copy(acc_ref.at[:, pl.ds(acc_start, b_ref.shape[1])], acc_buf, sems.at[2])
        l_copy.start()
        b_copy.start()
        acc_copy.start()
        l_copy.wait()
        b_copy.wait()
        acc_copy.wait()

        @pl.loop(0, b_ref.shape[1] // tile)
        def _(n):
            columns = pl.ds(pl.multiple_of(n * tile, tile), tile)
            acc = acc_buf[:, columns] + jnp.dot(l_buf[...], b_buf[:, columns], preferred_element_type=jnp.float32)
            out_buf[:, columns] = acc.astype(out_buf.dtype)

        out_copy = pltpu.make_async_copy(out_buf, x_ref.at[rows, pl.ds(start, b_ref.shape[1])], sems.at[3])
        out_copy.start()
        out_copy.wait()


def finish(step, start, row, l_last, piece, acc, acc_start, x):
    width = piece.shape[1]
    return pl.pallas_call(
        functools.partial(finish_kernel, step, start, row, 512 if width % 512 == 0 else 256, acc_start),
        in_specs=[pl.BlockSpec(memory_space=pltpu.HBM)] * 4,
        out_specs=pl.BlockSpec(memory_space=pltpu.HBM),
        out_shape=jax.ShapeDtypeStruct(x.shape, x.dtype),
        scratch_shapes=[
            pltpu.VMEM((BLOCK, BLOCK), l_last.dtype),
            pltpu.VMEM((BLOCK, width), piece.dtype),
            pltpu.VMEM((BLOCK, width), acc.dtype),
            pltpu.VMEM((BLOCK, width), x.dtype),
            pltpu.SemaphoreType.DMA((4,)),
        ],
        input_output_aliases={3: 0},
        compiler_params=pltpu.CompilerParams(vmem_limit_bytes=12 << 20),
        cost_estimate=pl.CostEstimate(
            flops=2 * BLOCK * BLOCK * width, bytes_accessed=BLOCK * width * 8, transcendentals=0),
    )(l_last, piece, acc, x)


def last_kernel(step, start, row, l_ref, b_ref, acc_ref, x_in, x_ref, out_buf, sem):
    del x_in

    @pl.when(lax.axis_index("row") == row)
    def _():
        acc = acc_ref[...] + jnp.dot(l_ref[...], b_ref[...], preferred_element_type=jnp.float32)
        out_buf[...] = acc.astype(out_buf.dtype)
        copy = pltpu.make_async_copy(
            out_buf, x_ref.at[pl.ds(step * BLOCK, BLOCK), pl.ds(start, b_ref.shape[1])], sem)
        copy.start()
        copy.wait()


def finish_last(step, start, row, l_last, piece, acc, x):
    width = piece.shape[1]
    return pl.pallas_call(
        functools.partial(last_kernel, step, start, row),
        in_specs=[pl.BlockSpec(memory_space=pltpu.VMEM)] * 3 + [pl.BlockSpec(memory_space=pltpu.HBM)],
        out_specs=pl.BlockSpec(memory_space=pltpu.HBM),
        out_shape=jax.ShapeDtypeStruct(x.shape, x.dtype),
        scratch_shapes=[pltpu.VMEM((BLOCK, width), x.dtype), pltpu.SemaphoreType.DMA],
        input_output_aliases={3: 0},
        compiler_params=pltpu.CompilerParams(vmem_limit_bytes=8 << 20),
        cost_estimate=pl.CostEstimate(
            flops=2 * BLOCK * BLOCK * width, bytes_accessed=BLOCK * width * 8, transcendentals=0),
    )(l_last, piece, acc, x)


def cut_kernel(row, start, b_ref, out_ref, sem):
    @pl.when(lax.axis_index("row") == 0)
    def _():
        copy = pltpu.make_async_copy(b_ref.at[pl.ds(row, BLOCK), pl.ds(start, out_ref.shape[1])], out_ref, sem)
        copy.start()
        copy.wait()


def cut(b, row, start, width):
    return pl.pallas_call(
        functools.partial(cut_kernel, row, start),
        in_specs=[pl.BlockSpec(memory_space=pltpu.HBM)],
        out_specs=pl.BlockSpec(memory_space=pl.ANY),
        out_shape=jax.ShapeDtypeStruct((BLOCK, width), b.dtype),
        scratch_shapes=[pltpu.SemaphoreType.DMA],
        compiler_params=pltpu.CompilerParams(vmem_limit_bytes=48 << 20),
        cost_estimate=pl.CostEstimate(flops=2 * BLOCK * width, bytes_accessed=BLOCK * width * 4, transcendentals=0),
    )(b)


def keep_kernel(row, piece_ref, out_ref, sem):
    @pl.when(lax.axis_index("row") == row)
    def _():
        copy = pltpu.make_async_copy(piece_ref, out_ref, sem)
        copy.start()
        copy.wait()


def keep(row, piece):
    return pl.pallas_call(
        functools.partial(keep_kernel, row),
        in_specs=[pl.BlockSpec(memory_space=pltpu.VMEM)],
        out_specs=pl.BlockSpec(memory_space=pltpu.HBM),
        out_shape=jax.ShapeDtypeStruct(piece.shape, piece.dtype),
        scratch_shapes=[pltpu.SemaphoreType.DMA],
        compiler_params=pltpu.CompilerParams(vmem_limit_bytes=1 << 20),
        cost_estimate=pl.CostEstimate(flops=2 * piece.size, bytes_accessed=4 * piece.size, transcendentals=0),
    )(piece)


def cut_rest_kernel(places, b_ref, *refs):
    count = len(places)
    out_refs, (head, body, fetch_sems, store_sems) = refs[:count], refs[count:]
    first_row, first_start, first_width = places[0]
    fetches = [pltpu.make_async_copy(b_ref.at[pl.ds(first_row, BLOCK), pl.ds(first_start, first_width)], head, fetch_sems.at[0])]
    stores = [pltpu.make_async_copy(head, out_refs[0], store_sems.at[0])]
    if count > 1:
        fetches.append(pltpu.make_async_copy(b_ref.at[pl.ds(BLOCK, body.shape[0])], body, fetch_sems.at[1]))
        for i, (row, start, width) in list(enumerate(places))[1:]:
            piece = body.at[pl.ds(row - BLOCK, BLOCK), pl.ds(start, width)]
            stores.append(pltpu.make_async_copy(piece, out_refs[i], store_sems.at[i]))
    for fetch in fetches:
        fetch.start()
    fetches[0].wait()
    stores[0].start()
    if count > 1:
        fetches[1].wait()
    for store in stores[1:]:
        store.start()
    for store in stores:
        store.wait()


def cut_rest(b, places):
    size = sum(width for _, _, width in places) * BLOCK
    body = (b.shape[0] - BLOCK, b.shape[1]) if len(places) > 1 else (BLOCK, BLOCK)
    return pl.pallas_call(
        functools.partial(cut_rest_kernel, places),
        in_specs=[pl.BlockSpec(memory_space=pltpu.HBM)],
        out_specs=[pl.BlockSpec(memory_space=pltpu.HBM)] * len(places),
        out_shape=[jax.ShapeDtypeStruct((BLOCK, width), b.dtype) for _, _, width in places],
        scratch_shapes=[
            pltpu.VMEM((BLOCK, places[0][2]), b.dtype),
            pltpu.VMEM(body, b.dtype),
            pltpu.SemaphoreType.DMA((2,)),
            pltpu.SemaphoreType.DMA((len(places),)),
        ],
        compiler_params=pltpu.CompilerParams(vmem_limit_bytes=48 << 20),
        cost_estimate=pl.CostEstimate(flops=2 * size, bytes_accessed=4 * size, transcendentals=0),
    )(b)


def solution(mesh):
    grid_rows = mesh.shape["row"]
    grid_cols = mesh.shape["col"]
    swap_row = [(r, r ^ 1) for r in range(grid_rows)]
    down_row = [(r, r + 1) for r in range(grid_rows - 1)]

    def local_trmm(tri_loc, rhs_loc):
        rows, cols = rhs_loc.shape
        steps = rows // BLOCK
        final = steps - 1
        half = cols // 2
        first = cols // 16

        order = [(final, cols - first, first)]
        order += [(j, h * half, half) for j in range(final) for h in range(2)]
        tail, off = [], 0
        for w in (half, cols // 4, 3 * first // 2, first, first // 2):
            tail.append((off, w))
            off += w
        order += [(final, off, w) for off, w in tail]

        got = {}

        def send(i, piece):
            j, off, _ = order[i]
            got[j, off] = lax.ppermute(piece, "row", down_row if i and j == final else swap_row)

        places = [(j * BLOCK, off, w) for j, off, w in order]
        piece = cut(rhs_loc, *places[0])
        send(0, piece)
        piece, = cut_rest(rhs_loc, places[1:2])
        send(1, piece)
        pieces = cut_rest(rhs_loc, places[2:-1])
        for i, piece in enumerate(pieces):
            send(2 + i, piece)
        got[final, cols - first] = keep(grid_rows - 1, got[final, cols - first])
        l_core, l_chip, l_both = (
            lax.ppermute(tri_loc, "col", [(c, c ^ d) for c in range(grid_cols)]) for d in (1, 2, 3))
        l_parts = [tri_loc, l_core, l_chip, l_both]

        x, acc = None, [None, None]
        for h in range(2):
            early = got[final, cols - first] if h == 1 else None
            x, acc[h], l_last = bulk(h * half, first, l_parts, rhs_loc, [got[k, h * half] for k in range(final)], early, x)
        off, w = tail[-1]
        acc_last = acc[1][:, off - half:off - half + w]
        source, acc[1] = lax.optimization_barrier((rhs_loc, acc[1]))
        send(len(order) - 1, source[final * BLOCK:, off:off + w])
        for off, w in tail[:-1]:
            h = off // half
            x = finish(final, off, grid_rows - 1, l_last, got[final, off], acc[h], off - h * half, x)
        off, w = tail[-1]
        return finish_last(final, off, grid_rows - 1, l_last, got[final, off], acc_last, x)

    part_spec = P(("batch", "row"), "col")
    return jax.shard_map(local_trmm, mesh=mesh, in_specs=(part_spec, part_spec), out_specs=part_spec, check_vma=False)
```

```python
import functools

import jax
import jax.numpy as jnp
from jax import lax
from jax.experimental import pallas as pl
from jax.experimental.pallas import tpu as pltpu
from jax.sharding import PartitionSpec as P


BLOCK = 256


def bulk_kernel(steps, aliased, early, *refs):
    l_refs, bo_ref, rem_refs = refs[:4], refs[4], refs[5:4 + steps]
    x_ref, acc_ref, last_ref, l_buf, sems = refs[4 + steps + aliased + early:]

    @pl.when(pl.program_id(0) == 0)
    def _():
        row, col = lax.axis_index("row"), lax.axis_index("col")
        copies = []
        for d in range(4):
            chip, core = (col // 2 + d // 2) % 2, (col + d) % 2
            side = (core + row) % 2
            for j in range(steps // 2):
                place = pl.multiple_of((2 * j + chip) * BLOCK, BLOCK)
                copies.append(pltpu.make_async_copy(
                    l_refs[d].at[:, pl.ds(j * BLOCK, BLOCK)], l_buf.at[side, :, pl.ds(place, BLOCK)], sems.at[len(copies)]))
        for copy in copies:
            copy.start()
        for copy in copies:
            copy.wait()
        last_ref[...] = l_buf[1, (steps - 1) * BLOCK:, (steps - 1) * BLOCK:]

    for step in range(steps):
        rows = slice(step * BLOCK, (step + 1) * BLOCK)
        depth = (step + 1) * BLOCK
        acc = jnp.dot(l_buf[0, rows, :depth], bo_ref[:depth, :], preferred_element_type=jnp.float32)
        for j in range(min(step + 1, steps - 1)):
            columns = slice(j * BLOCK, (j + 1) * BLOCK)
            acc += jnp.dot(l_buf[1, rows, columns], rem_refs[j][...], preferred_element_type=jnp.float32)
        x_ref[rows, :] = acc.astype(x_ref.dtype)
    acc_ref[...] = acc

    if early:
        early_ref = refs[4 + steps]

        @pl.when((pl.program_id(0) == pl.num_programs(0) - 1) & (lax.axis_index("row") == 1))
        def _():
            done = acc_ref[...] + jnp.dot(last_ref[...], early_ref[...], preferred_element_type=jnp.float32)
            x_ref[(steps - 1) * BLOCK:, :] = done.astype(x_ref.dtype)


def bulk(start, tile, l_parts, b_own, pieces, early, x):
    rows, cols = b_own.shape
    steps = rows // BLOCK
    width = pieces[0].shape[1]
    base = start // tile
    column = pl.BlockSpec((rows, tile), lambda n: (0, base + n))
    in_specs = [pl.BlockSpec(memory_space=pltpu.HBM)] * 4 + [column]
    in_specs += [pl.BlockSpec((BLOCK, tile), lambda n: (0, n))] * (steps - 1)
    args = [*l_parts, b_own, *pieces]
    if early is not None:
        args.append(early)
        in_specs.append(pl.BlockSpec((BLOCK, tile), lambda n: (0, 0)))
    aliases = {}
    if x is not None:
        aliases = {len(args): 0}
        args.append(x)
        in_specs.append(pl.BlockSpec(memory_space=pltpu.HBM))
    return pl.pallas_call(
        functools.partial(bulk_kernel, steps, len(aliases), int(early is not None)),
        grid=(width // tile,),
        in_specs=in_specs,
        out_specs=[column, pl.BlockSpec((BLOCK, tile), lambda n: (0, n)), pl.BlockSpec((BLOCK, BLOCK), lambda n: (0, 0))],
        out_shape=[
            jax.ShapeDtypeStruct((rows, cols), jnp.bfloat16),
            jax.ShapeDtypeStruct((BLOCK, width), jnp.float32),
            jax.ShapeDtypeStruct((BLOCK, BLOCK), jnp.bfloat16),
        ],
        scratch_shapes=[pltpu.VMEM((2, rows, rows), jnp.bfloat16), pltpu.SemaphoreType.DMA((2 * steps,))],
        input_output_aliases=aliases,
        compiler_params=pltpu.CompilerParams(vmem_limit_bytes=60 << 20),
        cost_estimate=pl.CostEstimate(
            flops=2 * rows * rows * width, bytes_accessed=3 * rows * width * 2, transcendentals=0),
    )(*args)


def finish_kernel(step, start, row, tile, acc_start, l_ref, b_ref, acc_ref, x_in, x_ref, l_buf, b_buf, acc_buf, out_buf, sems):
    del x_in
    rows = pl.ds(step * BLOCK, BLOCK)

    @pl.when(lax.axis_index("row") == row)
    def _():
        l_copy = pltpu.make_async_copy(l_ref, l_buf, sems.at[0])
        b_copy = pltpu.make_async_copy(b_ref, b_buf, sems.at[1])
        acc_copy = pltpu.make_async_copy(acc_ref.at[:, pl.ds(acc_start, b_ref.shape[1])], acc_buf, sems.at[2])
        l_copy.start()
        b_copy.start()
        acc_copy.start()
        l_copy.wait()
        b_copy.wait()
        acc_copy.wait()

        @pl.loop(0, b_ref.shape[1] // tile)
        def _(n):
            columns = pl.ds(pl.multiple_of(n * tile, tile), tile)
            acc = acc_buf[:, columns] + jnp.dot(l_buf[...], b_buf[:, columns], preferred_element_type=jnp.float32)
            out_buf[:, columns] = acc.astype(out_buf.dtype)

        out_copy = pltpu.make_async_copy(out_buf, x_ref.at[rows, pl.ds(start, b_ref.shape[1])], sems.at[3])
        out_copy.start()
        out_copy.wait()


def finish(step, start, row, l_last, piece, acc, acc_start, x):
    width = piece.shape[1]
    return pl.pallas_call(
        functools.partial(finish_kernel, step, start, row, 512 if width % 512 == 0 else 256, acc_start),
        in_specs=[pl.BlockSpec(memory_space=pltpu.HBM)] * 4,
        out_specs=pl.BlockSpec(memory_space=pltpu.HBM),
        out_shape=jax.ShapeDtypeStruct(x.shape, x.dtype),
        scratch_shapes=[
            pltpu.VMEM((BLOCK, BLOCK), l_last.dtype),
            pltpu.VMEM((BLOCK, width), piece.dtype),
            pltpu.VMEM((BLOCK, width), acc.dtype),
            pltpu.VMEM((BLOCK, width), x.dtype),
            pltpu.SemaphoreType.DMA((4,)),
        ],
        input_output_aliases={3: 0},
        compiler_params=pltpu.CompilerParams(vmem_limit_bytes=12 << 20),
        cost_estimate=pl.CostEstimate(
            flops=2 * BLOCK * BLOCK * width, bytes_accessed=BLOCK * width * 8, transcendentals=0),
    )(l_last, piece, acc, x)


def last_kernel(step, start, row, l_ref, b_ref, acc_ref, x_in, x_ref, out_buf, sem):
    del x_in

    @pl.when(lax.axis_index("row") == row)
    def _():
        acc = acc_ref[...] + jnp.dot(l_ref[...], b_ref[...], preferred_element_type=jnp.float32)
        out_buf[...] = acc.astype(out_buf.dtype)
        copy = pltpu.make_async_copy(
            out_buf, x_ref.at[pl.ds(step * BLOCK, BLOCK), pl.ds(start, b_ref.shape[1])], sem)
        copy.start()
        copy.wait()


def finish_last(step, start, row, l_last, piece, acc, x):
    width = piece.shape[1]
    return pl.pallas_call(
        functools.partial(last_kernel, step, start, row),
        in_specs=[pl.BlockSpec(memory_space=pltpu.VMEM)] * 3 + [pl.BlockSpec(memory_space=pltpu.HBM)],
        out_specs=pl.BlockSpec(memory_space=pltpu.HBM),
        out_shape=jax.ShapeDtypeStruct(x.shape, x.dtype),
        scratch_shapes=[pltpu.VMEM((BLOCK, width), x.dtype), pltpu.SemaphoreType.DMA],
        input_output_aliases={3: 0},
        compiler_params=pltpu.CompilerParams(vmem_limit_bytes=8 << 20),
        cost_estimate=pl.CostEstimate(
            flops=2 * BLOCK * BLOCK * width, bytes_accessed=BLOCK * width * 8, transcendentals=0),
    )(l_last, piece, acc, x)


def cut_kernel(row, start, b_ref, out_ref, sem):
    @pl.when(lax.axis_index("row") == 0)
    def _():
        copy = pltpu.make_async_copy(b_ref.at[pl.ds(row, BLOCK), pl.ds(start, out_ref.shape[1])], out_ref, sem)
        copy.start()
        copy.wait()


def cut(b, row, start, width):
    return pl.pallas_call(
        functools.partial(cut_kernel, row, start),
        in_specs=[pl.BlockSpec(memory_space=pltpu.HBM)],
        out_specs=pl.BlockSpec(memory_space=pl.ANY),
        out_shape=jax.ShapeDtypeStruct((BLOCK, width), b.dtype),
        scratch_shapes=[pltpu.SemaphoreType.DMA],
        compiler_params=pltpu.CompilerParams(vmem_limit_bytes=48 << 20),
        cost_estimate=pl.CostEstimate(flops=2 * BLOCK * width, bytes_accessed=BLOCK * width * 4, transcendentals=0),
    )(b)


def keep_kernel(row, piece_ref, out_ref, sem):
    @pl.when(lax.axis_index("row") == row)
    def _():
        copy = pltpu.make_async_copy(piece_ref, out_ref, sem)
        copy.start()
        copy.wait()


def keep(row, piece):
    return pl.pallas_call(
        functools.partial(keep_kernel, row),
        in_specs=[pl.BlockSpec(memory_space=pltpu.VMEM)],
        out_specs=pl.BlockSpec(memory_space=pltpu.HBM),
        out_shape=jax.ShapeDtypeStruct(piece.shape, piece.dtype),
        scratch_shapes=[pltpu.SemaphoreType.DMA],
        compiler_params=pltpu.CompilerParams(vmem_limit_bytes=1 << 20),
        cost_estimate=pl.CostEstimate(flops=2 * piece.size, bytes_accessed=4 * piece.size, transcendentals=0),
    )(piece)


def cut_many_kernel(places, b_ref, *refs):
    count = len(places)
    out_refs, bufs, sems = refs[:count], refs[count:2 * count], refs[2 * count]
    fetches = [
        pltpu.make_async_copy(b_ref.at[pl.ds(row, BLOCK), pl.ds(start, width)], bufs[i], sems.at[0, i])
        for i, (row, start, width) in enumerate(places)]
    stores = [pltpu.make_async_copy(bufs[i], out_refs[i], sems.at[1, i]) for i in range(count)]
    for fetch in fetches:
        fetch.start()
    for fetch, store in zip(fetches, stores):
        fetch.wait()
        store.start()
    for store in stores:
        store.wait()


def cut_many(b, places):
    size = sum(width for _, _, width in places) * BLOCK
    return pl.pallas_call(
        functools.partial(cut_many_kernel, places),
        in_specs=[pl.BlockSpec(memory_space=pltpu.HBM)],
        out_specs=[pl.BlockSpec(memory_space=pltpu.HBM)] * len(places),
        out_shape=[jax.ShapeDtypeStruct((BLOCK, width), b.dtype) for _, _, width in places],
        scratch_shapes=[pltpu.VMEM((BLOCK, width), b.dtype) for _, _, width in places]
        + [pltpu.SemaphoreType.DMA((2, len(places)))],
        compiler_params=pltpu.CompilerParams(vmem_limit_bytes=48 << 20),
        cost_estimate=pl.CostEstimate(flops=2 * size, bytes_accessed=4 * size, transcendentals=0),
    )(b)


def solution(mesh):
    grid_rows = mesh.shape["row"]
    grid_cols = mesh.shape["col"]
    swap_row = [(r, r ^ 1) for r in range(grid_rows)]
    down_row = [(r, r + 1) for r in range(grid_rows - 1)]

    def local_trmm(tri_loc, rhs_loc):
        rows, cols = rhs_loc.shape
        steps = rows // BLOCK
        final = steps - 1
        half = cols // 2
        first = cols // 16

        order = [(final, cols - first, first)]
        order += [(j, h * half, half) for j in range(final) for h in range(2)]
        tail, off = [], 0
        for w in (half, cols // 4, 3 * first // 2, first, first // 2):
            tail.append((off, w))
            off += w
        order += [(final, off, w) for off, w in tail]

        got = {}

        def send(i, piece):
            j, off, _ = order[i]
            got[j, off] = lax.ppermute(piece, "row", down_row if i and j == final else swap_row)

        places = [(j * BLOCK, off, w) for j, off, w in order]
        piece = cut(rhs_loc, *places[0])
        send(0, piece)
        piece, = cut_many(rhs_loc, places[1:2])
        send(1, piece)
        pieces = cut_many(rhs_loc, places[2:-1])
        for i, piece in enumerate(pieces):
            send(2 + i, piece)
        got[final, cols - first] = keep(grid_rows - 1, got[final, cols - first])
        l_core, l_chip, l_both = (
            lax.ppermute(tri_loc, "col", [(c, c ^ d) for c in range(grid_cols)]) for d in (1, 2, 3))
        l_parts = [tri_loc, l_core, l_chip, l_both]

        x, acc = None, [None, None]
        for h in range(2):
            early = got[final, cols - first] if h == 1 else None
            x, acc[h], l_last = bulk(h * half, first, l_parts, rhs_loc, [got[k, h * half] for k in range(final)], early, x)
        off, w = tail[-1]
        acc_last = acc[1][:, off - half:off - half + w]
        source, acc[1] = lax.optimization_barrier((rhs_loc, acc[1]))
        send(len(order) - 1, source[final * BLOCK:, off:off + w])
        for off, w in tail[:-1]:
            h = off // half
            x = finish(final, off, grid_rows - 1, l_last, got[final, off], acc[h], off - h * half, x)
        off, w = tail[-1]
        return finish_last(final, off, grid_rows - 1, l_last, got[final, off], acc_last, x)

    part_spec = P(("batch", "row"), "col")
    return jax.shard_map(local_trmm, mesh=mesh, in_specs=(part_spec, part_spec), out_specs=part_spec, check_vma=False)
```
